32 devices in a mesh: grp: 2 (over x), gx: 4 (over z), gy: 4 (over y, core).
Axes of the slice: x: 2, y: 2, z: 4, core: 2. Of those that a mesh axis runs over, the one named last changes fastest.
Arguments:
- state: float32 [2, 3, 144, 192, 90], P('grp', None, 'gx', 'gy'), may hold values from -6 to 6
- courant: float32 [2, 144, 192, 90], P('grp', 'gx', 'gy'), may hold values from 0.15 to 0.5
- vert_inverse: float32 [2, 90, 90], P('grp'), may hold values from -0.1 to 0.65, as said below
- interp_index: int32 [144, 192, 4], P('gx', 'gy'), may hold values from 0 to 8
- interp_weight: float32 [144, 192, 4], P('gx', 'gy'), may hold values from 0.2 to 1
- restrict_index: int32 [48, 64, 9], P('gx', 'gy'), may hold values from 0 to 8
- restrict_weight: float32 [48, 64, 9], P('gx', 'gy'), may hold values from 0.2 to 1
Outputs:
- new_state: float32 [2, 3, 144, 192, 90], P('grp', None, 'gx', 'gy')
The draws below stay inside these ranges and needn't reach their ends.
Inputs may be any that keep to these rules, and one draw needn't show every extreme that they name: `vert_inverse`: each matrix's diagonal lies in 0.5 to 0.65, its neighbours on the diagonal beside it in 0.05 to 0.12, the rest is small.
All inputs are finite; a program needn't handle non-finite values.
Results may differ from the reference program's by a relative error of at most 0.0001.
Values sent between devices are 32-bit elements; how exact they have to be, the bound alone decides.
A program may use at most 128 MiB of HBM per device.

```python
import math
import jax
import jax.numpy as jnp
from jax import lax

LEV = 90
SUBS = 4
BAND = 5
NK = 9
NX = 144
NY = 192
FX = 48
FY = 64
OX = 72
OY = 96


def draw_vert_inverse(key, part):
    keys = jax.random.split(key, 3)
    diagonal = jax.random.uniform(keys[0], (2, LEV), jnp.float32, 0.5, 0.65)
    beside = jax.random.uniform(keys[1], (2, LEV - 1), jnp.float32, 0.05, 0.12)
    beside = jnp.pad(beside, ((0, 0), (0, 1)))
    upper = beside[:, :, None] * jnp.eye(LEV, k=1, dtype=jnp.float32)[None]
    noise = jax.random.normal(keys[2], (2, LEV, LEV), jnp.float32) * (0.01 / jnp.sqrt(1.0 * LEV))
    noise = jnp.clip(noise, -0.02, 0.02)
    matrix = diagonal[:, :, None] * jnp.eye(LEV, dtype=jnp.float32)[None] + upper + jnp.swapaxes(upper, 1, 2) + noise
    return matrix.astype(jnp.float32)


def plant(array, key, least, largest):
    spot = [jax.random.randint(jax.random.fold_in(key, axis), (), 0, length) for axis, length in enumerate(array.shape)]
    longest = array.shape.index(max(array.shape))
    neighbour = spot[:longest] + [(spot[longest] + 1) % array.shape[longest]] + spot[longest + 1:]
    return array.at[tuple(spot)].set(least).at[tuple(neighbour)].set(largest)


def level_of(own_key, extent, cuts, smallest, largest):
    loudness, own = 1.0, jax.random.fold_in(own_key, 6)
    for dim, blocks in cuts:
        steps = jnp.exp(jax.random.uniform(jax.random.fold_in(own, dim), (blocks,), jnp.float32, smallest / len(cuts), largest / len(cuts)))
        loudness = loudness * jnp.repeat(steps, extent[dim] // blocks).reshape([-1 if axis == dim else 1 for axis in range(len(extent))])
    return loudness


def bell_draw(stream_key, shape, deviation, reach, cuts=(), kind=jnp.bfloat16):
    values = deviation * jax.random.normal(stream_key, shape, jnp.float32)
    if cuts:
        values = values * level_of(stream_key, shape, cuts, -0.22, 0.18)
    return jnp.clip(values, -reach, reach).astype(kind)


def setup_inputs(seed: int = 0) -> dict:
    key_of = jax.random.split(jax.random.key(seed), 8)
    state = bell_draw(key_of[0], (2, 3, NX, NY, LEV), 1.0, 6.0, ((0, 2), (2, 4), (3, 4)), jnp.float32)
    courant = jnp.clip(jnp.exp(math.log(0.5) - 1.2039728 * jax.random.uniform(key_of[1], (2, NX, NY, LEV), jnp.float32) ** level_of(key_of[1], (2, NX, NY, LEV), ((0, 2), (1, 4), (2, 4)), -0.2, 0.2)), 0.15, 0.5)
    vert_inverse = draw_vert_inverse(jax.random.fold_in(key_of[7], 71), 0)
    interp_index = plant(jax.random.randint(key_of[3], (NX, NY, 4), 0, 9), jax.random.fold_in(key_of[3], 1), 0, 8).astype(jnp.int32)
    interp_weight = jnp.clip(0.2 + 0.8 * jax.random.uniform(key_of[4], (NX, NY, 4), jnp.float32) ** level_of(key_of[4], (NX, NY, 4), ((0, 4), (1, 4)), -0.2, 0.2), 0.2, 1.0)
    restrict_index = plant(jax.random.randint(key_of[5], (FX, FY, NK), 0, 9), jax.random.fold_in(key_of[5], 1), 0, 8).astype(jnp.int32)
    restrict_weight = jnp.clip(0.2 + 0.8 * jax.random.uniform(key_of[6], (FX, FY, NK), jnp.float32) ** level_of(key_of[6], (FX, FY, NK), ((0, 4), (1, 4)), -0.2, 0.2), 0.2, 1.0)
    return dict(state=state, courant=courant, vert_inverse=vert_inverse, interp_index=interp_index, interp_weight=interp_weight, restrict_index=restrict_index, restrict_weight=restrict_weight)


FEEDBACK = 0.5


def slope_x(field):
    return 0.5 * (field[..., 2:, 1:-1, :] - field[..., :-2, 1:-1, :])


def slope_y(field):
    return 0.5 * (field[..., 1:-1, 2:, :] - field[..., 1:-1, :-2, :])


def padded(field):
    return jnp.pad(field, ((1, 1), (1, 1), (0, 0)))


def vertical(pressure, inverse):
    return jnp.einsum("xyk,kl->xyl", pressure, inverse, precision=lax.Precision.HIGHEST)


def substeps(fields, speed, inverse):
    pressure, wind_x, wind_y = fields[0], fields[1], fields[2]
    running = jnp.zeros_like(fields)
    for substep in range(SUBS):
        rimmed = padded(pressure)
        wind_x = wind_x - speed * slope_x(rimmed)
        wind_y = wind_y - speed * slope_y(rimmed)
        pressure = pressure - speed * (slope_x(padded(wind_x)) + slope_y(padded(wind_y)))
        pressure = vertical(pressure, inverse)
        running = running + jnp.stack([pressure, wind_x, wind_y])
    return jnp.stack([pressure, wind_x, wind_y]), running / SUBS


def weighted_sum(source, child_rows, child_cols, weight):
    shares = weight / jnp.sum(weight, axis=-1, keepdims=True)
    summed = jnp.zeros((source.shape[0],) + child_rows.shape[:2] + (source.shape[-1],), jnp.float32)
    for term in range(child_rows.shape[2]):
        summed = summed + shares[None, :, :, term, None] * source[:, child_rows[:, :, term], child_cols[:, :, term], :]
    return summed


def reference(state, courant, vert_inverse, interp_index, interp_weight, restrict_index, restrict_weight):
    parent_end, parent_mean = substeps(state[0], courant[0], vert_inverse[0])
    nest_end, nest_mean = substeps(state[1], courant[1], vert_inverse[1])
    fine_x = jnp.arange(NX, dtype=jnp.int32)
    fine_y = jnp.arange(NY, dtype=jnp.int32)
    source_x = jnp.clip((OX - 1 + fine_x // 3)[:, None, None] + interp_index // 3, OX, OX + FX - 1).astype(jnp.int32)
    source_y = jnp.clip((OY - 1 + fine_y // 3)[None, :, None] + interp_index % 3, OY, OY + FY - 1).astype(jnp.int32)
    boundary = weighted_sum(parent_end, source_x, source_y, interp_weight)
    coarse_x = jnp.arange(FX, dtype=jnp.int32)
    coarse_y = jnp.arange(FY, dtype=jnp.int32)
    child_x = (3 * coarse_x)[:, None, None] + restrict_index // 3
    child_y = (3 * coarse_y)[None, :, None] + restrict_index % 3
    footprint = weighted_sum(nest_mean, child_x, child_y, restrict_weight)
    restricted = jnp.zeros_like(parent_end).at[:, OX:OX + FX, OY:OY + FY, :].set(footprint)
    column_x = fine_x[:, None]
    column_y = fine_y[None, :]
    edge_depth = jnp.minimum(jnp.minimum(column_x, NX - 1 - column_x), jnp.minimum(column_y, NY - 1 - column_y)).astype(jnp.float32)
    relax_weight = jnp.maximum(1.0 - edge_depth / BAND, 0.0)[None, :, :, None]
    nest_new = nest_end + relax_weight * (boundary - nest_end)
    region = ((column_x >= OX) & (column_x < OX + FX) & (column_y >= OY) & (column_y < OY + FY)).astype(jnp.float32)[None, :, :, None]
    parent_new = parent_end + FEEDBACK * region * (restricted - parent_end)
    return jnp.stack([parent_new, nest_new])
```

```python
import functools

import jax
import jax.numpy as jnp
from jax import lax
from jax.experimental import pallas as pl
from jax.experimental.pallas import tpu as pltpu
from jax.sharding import PartitionSpec as P

SUBS = 4
BAND = 5
FEEDBACK = 0.5
MESH = pl.DeviceIdType.MESH
F32 = jnp.float32
XB, YB = 2, 8


def split(a):
    high = a.astype(jnp.bfloat16)
    return high, (a - high.astype(F32)).astype(jnp.bfloat16)


def dot(a, b):
    return jnp.dot(a, b, preferred_element_type=F32)


def dot3(a, b_high, b_low):
    a_high, a_low = split(a)
    return dot(a_high, b_high) + (dot(a_low, b_high) + dot(a_high, b_low))


def third(t):
    return (t * 11) >> 5


def dense(cell, share, depth):
    lanes = lax.broadcasted_iota(jnp.int32, (cell.shape[0], depth), 1)
    total = jnp.zeros(lanes.shape, F32)
    for k in range(cell.shape[1]):
        total = total + jnp.where(lanes == cell[:, k : k + 1], share[:, k : k + 1], 0.0)
    return total


def kernel(
    cx, cy,
    state, courant, inverse, iidx, iwgt, ridx, rwgt,
    out,
    S, C, mean, sx0, sy0, rx0, ry0, sx, sy, rx, ry, rst, fb, xstrip, ystrip,
    load_sem, halo_send, halo_recv, strip_send, strip_recv, fb_send, fb_recv, out_sem,
):
    g, a, b = lax.axis_index("grp"), lax.axis_index("gx"), lax.axis_index("gy")
    nx, ny, lev = state.shape[2], state.shape[3], state.shape[4]
    tx, ty = nx // 3, ny // 3
    fx, fy = cx // 2, cy // 2

    loads = [
        pltpu.make_async_copy(
            state.at[0], S.at[:, pl.ds(XB, nx), pl.ds(YB, ny), :], load_sem.at[0]
        ),
        pltpu.make_async_copy(
            courant.at[0], C.at[pl.ds(1, nx), pl.ds(YB, ny), :], load_sem.at[1]
        ),
    ]
    for copy in loads:
        copy.start()
    zrow = jnp.zeros((2, ny, lev), F32)
    S[0, 0:2, YB : YB + ny, :] = zrow
    S[0, XB + nx : XB + nx + 2, YB : YB + ny, :] = zrow
    S[1, 0:2, YB : YB + ny, :] = zrow
    S[1, XB + nx : XB + nx + 2, YB : YB + ny, :] = zrow
    C[0:1, YB : YB + ny, :] = zrow[0:1]
    C[nx + 1 : nx + 2, YB : YB + ny, :] = zrow[0:1]
    zcol = jnp.zeros((nx, 8, lev), F32)
    for c in (0, 2):
        S[c, XB : XB + nx, 0:YB, :] = zcol
        S[c, XB : XB + nx, YB + ny : YB + ny + 8, :] = zcol
    C[1 : 1 + nx, 0:YB, :] = zcol
    C[1 : 1 + nx, YB + ny : YB + ny + 8, :] = zcol
    m_high, m_low = split(inverse[0])
    for copy in loads:
        copy.wait()

    dirs = (
        (a > 0, a < cx - 1, (g, a - 1, b)),
        (a < cx - 1, a > 0, (g, a + 1, b)),
        (b > 0, b < cy - 1, (g, a, b - 1)),
        (b < cy - 1, b > 0, (g, a, b + 1)),
    )

    def halo_copy(k, d):
        if k == 0:
            src, dst = (sx0, rx0) if d < 2 else (sy0, ry0)
            src, dst = src.at[d % 2], dst.at[d % 2]
        else:
            src, dst = (sx, rx) if d < 2 else (sy, ry)
            src, dst = src.at[k - 1, d % 2], dst.at[k - 1, d % 2]
        return pltpu.make_async_remote_copy(
            src_ref=src, dst_ref=dst,
            send_sem=halo_send.at[k, d], recv_sem=halo_recv.at[k, d],
            device_id=dirs[d][2], device_id_type=MESH,
        )

    def exchange(k):
        cols = slice(YB, YB + ny)
        rows = slice(XB, XB + nx)
        last_x, last_y = XB + nx, YB + ny
        if k == 0:
            sx0[0, 0:2] = S[0, XB : XB + 2, cols, :]
            sx0[0, 2:3] = S[1, XB : XB + 1, cols, :]
            sx0[0, 3:4] = C[1:2, cols, :]
            sx0[1, 0:2] = S[0, last_x - 2 : last_x, cols, :]
            sx0[1, 2:3] = S[1, last_x - 1 : last_x, cols, :]
            sx0[1, 3:4] = C[nx : nx + 1, cols, :]
            sy0[0, :, 0:2] = S[0, rows, YB : YB + 2, :]
            sy0[0, :, 2:3] = S[2, rows, YB : YB + 1, :]
            sy0[0, :, 3:4] = C[1 : 1 + nx, YB : YB + 1, :]
            sy0[1, :, 0:2] = S[0, rows, last_y - 2 : last_y, :]
            sy0[1, :, 2:3] = S[2, rows, last_y - 1 : last_y, :]
            sy0[1, :, 3:4] = C[1 : 1 + nx, last_y - 1 : last_y, :]
        else:
            sx[k - 1, 0] = S[0, XB : XB + 2, cols, :]
            sx[k - 1, 1] = S[0, last_x - 2 : last_x, cols, :]
            sy[k - 1, 0] = S[0, rows, YB : YB + 2, :]
            sy[k - 1, 1] = S[0, rows, last_y - 2 : last_y, :]
        for d in range(4):
            @pl.when(dirs[d][0])
            def _():
                halo_copy(k, d).start()
        for d in range(4):
            @pl.when(dirs[d][1])
            def _():
                halo_copy(k, d).wait_recv()
                if d < 2:
                    got = rx0.at[d] if k == 0 else rx.at[k - 1, d]
                    at = last_x if d == 0 else XB - 2
                    S[0, at : at + 2, cols, :] = got[0:2]
                    if k == 0:
                        at = last_x if d == 0 else XB - 1
                        S[1, at : at + 1, cols, :] = got[2:3]
                        C[at - 1 : at, cols, :] = got[3:4]
                else:
                    got = ry0.at[d - 2] if k == 0 else ry.at[k - 1, d - 2]
                    at = last_y if d == 2 else YB - 2
                    S[0, rows, at : at + 2, :] = got[:, 0:2]
                    if k == 0:
                        at = last_y if d == 2 else YB - 1
                        S[2, rows, at : at + 1, :] = got[:, 2:3]
                        C[1 : 1 + nx, at : at + 1, :] = got[:, 3:4]

    def add_mean(k, c, x, value):
        mean[c, x] = value if k == 0 else mean[c, x] + value

    def winds(k):
        def u_row(r, _):
            slope = 0.5 * (S[0, r + 1, YB : YB + ny, :] - S[0, r - 1, YB : YB + ny, :])
            S[1, r, YB : YB + ny, :] = S[1, r, YB : YB + ny, :] - C[r - 1, YB : YB + ny, :] * slope
            return 0

        u_row(XB - 1, 0)
        u_row(XB + nx, 0)

        def row(x, _):
            r = x + XB
            u_row(r, 0)
            add_mean(k, 1, x, S[1, r, YB : YB + ny, :])
            wide = slice(YB - 1, YB + ny + 1)
            slope = 0.5 * (S[0, r, YB : YB + ny + 2, :] - S[0, r, YB - 2 : YB + ny, :])
            S[2, r, wide, :] = S[2, r, wide, :] - C[x + 1, wide, :] * slope
            add_mean(k, 2, x, S[2, r, YB : YB + ny, :])
            return 0

        lax.fori_loop(0, nx, row, 0)

    def press(k):
        group = 4

        def rows(i, _):
            parts = []
            for j in range(group):
                x = i * group + j
                r = x + XB
                div = 0.5 * (S[1, r + 1, YB : YB + ny, :] - S[1, r - 1, YB : YB + ny, :]) + 0.5 * (
                    S[2, r, YB + 1 : YB + ny + 1, :] - S[2, r, YB - 1 : YB + ny - 1, :]
                )
                parts.append(S[0, r, YB : YB + ny, :] - C[x + 1, YB : YB + ny, :] * div)
            solved = dot3(jnp.concatenate(parts, axis=0), m_high, m_low)
            for j in range(group):
                x = i * group + j
                new = solved[j * ny : (j + 1) * ny]
                S[0, x + XB, YB : YB + ny, :] = new
                add_mean(k, 0, x, new)
            return 0

        lax.fori_loop(0, nx // group, rows, 0)

    slot = (a % 3) * 3 + b % 3

    def fb_copy(c):
        return pltpu.make_async_remote_copy(
            src_ref=rst.at[c], dst_ref=fb.at[slot, c],
            send_sem=fb_send.at[c], recv_sem=fb_recv.at[slot, c],
            device_id=(0, fx + a // 3, fy + b // 3), device_id_type=MESH,
        )

    def restrict(comps):
        def row(u, _):
            t = ridx[u]
            w = rwgt[u]
            share = w * (1.0 / SUBS) / jnp.sum(w, axis=-1, keepdims=True)
            over = third(t)
            cell = over * ny + (t - 3 * over) + 3 * lax.broadcasted_iota(jnp.int32, t.shape, 0)
            w_high, w_low = split(dense(cell, share, 3 * ny))
            for c in comps:
                block = mean[c, pl.ds(3 * u, 3)].reshape(3 * ny, lev)
                b_high, b_low = split(block)
                rst[c, u] = dot(w_high, b_high) + (dot(w_low, b_high) + dot(w_high, b_low))
            return 0

        lax.fori_loop(0, tx, row, 0)

    for k in range(SUBS):
        exchange(k)
        winds(k)
        if k == SUBS - 1:
            @pl.when(g == 1)
            def _():
                restrict((1, 2))
                fb_copy(1).start()
                fb_copy(2).start()
        press(k)

    x_windows = {-1: (0, 8, 24), 0: (0, ty + 8, 8), 1: (ty - 8, 2 * ty + 8, 0),
                 2: (2 * ty - 8, ny, 0), 3: (ny - 8, ny, 0)}
    y_windows = {-1: (0, 1, tx + 1), 0: (0, tx + 1, 1), 1: (tx - 1, 2 * tx + 1, 0),
                 2: (2 * tx - 1, nx, 0), 3: (nx - 1, nx, 0)}
    kinds = {-1: 1, 0: 0, 1: 0, 2: 0, 3: 2}

    def strip_copies():
        for side in range(2):
            edge = 0 if side == 0 else cx - 1
            at = XB if side == 0 else XB + tx * (edge % 3) + tx - 3
            for j in range(-1, 4):
                lo, hi, dst = x_windows[j]
                child = 3 * (b - fy) + j
                on = (a == fx + edge // 3) & (b >= fy) & (child >= 0) & (child < cy)
                yield on, pltpu.make_async_remote_copy(
                    src_ref=S.at[:, pl.ds(at, 3), pl.ds(YB + lo, hi - lo), :],
                    dst_ref=xstrip.at[:, :, pl.ds(dst, hi - lo), :],
                    send_sem=strip_send.at[0, side, j + 1], recv_sem=strip_recv.at[0, kinds[j]],
                    device_id=(1, edge, child), device_id_type=MESH,
                )
            edge = 0 if side == 0 else cy - 1
            at = YB if side == 0 else YB + ty * (edge % 3) + ty - 8
            for i in range(-1, 4):
                lo, hi, dst = y_windows[i]
                child = 3 * (a - fx) + i
                on = (b == fy + edge // 3) & (a >= fx) & (child >= 0) & (child < cx)
                yield on, pltpu.make_async_remote_copy(
                    src_ref=S.at[:, pl.ds(XB + lo, hi - lo), pl.ds(at, 8), :],
                    dst_ref=ystrip.at[:, pl.ds(dst, hi - lo), :, :],
                    send_sem=strip_send.at[1, side, i + 1], recv_sem=strip_recv.at[1, kinds[i]],
                    device_id=(1, child, edge), device_id_type=MESH,
                )

    def strip_wait(axis, kind, lo, hi, dst):
        if axis == 0:
            ref = xstrip.at[:, :, pl.ds(dst, hi - lo), :]
        else:
            ref = ystrip.at[:, pl.ds(dst, hi - lo), :, :]
        pltpu.make_async_remote_copy(
            src_ref=ref, dst_ref=ref, send_sem=strip_send.at[0, 0, 0],
            recv_sem=strip_recv.at[axis, kind], device_id=(g, a, b), device_id_type=MESH,
        ).wait_recv()

    def wait_strips(axis, place, count, windows):
        for i in range(3):
            @pl.when(place % 3 == i)
            def _():
                strip_wait(axis, 0, *windows[i])

        @pl.when((place % 3 == 2) & (place < count - 1))
        def _():
            strip_wait(axis, 1, *windows[-1])

        @pl.when((place % 3 == 0) & (place > 0))
        def _():
            strip_wait(axis, 2, *windows[3])

    def relax_at(x, y):
        gx, gy = a * nx + x, b * ny + y
        depth = jnp.minimum(
            jnp.minimum(gx, nx * cx - 1 - gx), jnp.minimum(gy, ny * cy - 1 - gy)
        ).astype(F32)
        return jnp.maximum(1.0 - depth / BAND, 0.0)

    def shares_of(w):
        return w / jnp.sum(w, axis=-1, keepdims=True)

    def y_edge(col, strip0):
        def row(u, _):
            t = iidx[pl.ds(3 * u, 3), pl.ds(col, 8), :].reshape(24, 4)
            share = shares_of(iwgt[pl.ds(3 * u, 3), pl.ds(col, 8), :].reshape(24, 4))
            over = third(t)
            n = lax.broadcasted_iota(jnp.int32, (24, 4), 0)
            source_x = jnp.clip(a * tx + u + over - 1, 0, cx * tx - 1) - (a * tx + u - 1)
            y = col + (n & 7)
            y3 = (y * 171) >> 9
            source_y = jnp.clip(b * ty + y3 + (t - 3 * over) - 1, 0, cy * ty - 1) - (b * ty + strip0)
            w_high, w_low = split(dense(source_x * 8 + source_y, share, 24))
            n = lax.broadcasted_iota(jnp.int32, (24, lev), 0)
            relax = relax_at(3 * u + (n >> 3), col + (n & 7))
            for c in range(3):
                s_high, s_low = split(ystrip[c, pl.ds(u, 3)].reshape(24, lev))
                bound = dot(w_high, s_high) + (dot(w_low, s_high) + dot(w_high, s_low))
                at = (c, pl.ds(XB + 3 * u, 3), pl.ds(YB + col, 8), slice(None))
                now = S[at].reshape(24, lev)
                S[at] = (now + relax * (bound - now)).reshape(3, 8, lev)
            return 0

        lax.fori_loop(0, tx, row, 0)

    def x_edge(first, strip0):
        def row(i, _):
            x = first + i
            t = iidx[x]
            share = shares_of(iwgt[x])
            over = third(t)
            source_x = jnp.clip(a * tx + x // 3 + over - 1, 0, cx * tx - 1) - (a * tx + strip0)
            y = lax.broadcasted_iota(jnp.int32, (ny, 4), 0)
            y3 = (y * 171) >> 9
            source_y = jnp.clip(b * ty + y3 + (t - 3 * over) - 1, 0, cy * ty - 1) - (b * ty - 8)
            w_high, w_low = split(dense(source_x * (ty + 16) + source_y, share, 3 * (ty + 16)))
            y = lax.broadcasted_iota(jnp.int32, (ny, lev), 0)
            relax = relax_at(x, y)
            for c in range(3):
                s_high, s_low = split(xstrip[c].reshape(3 * (ty + 16), lev))
                bound = dot(w_high, s_high) + (dot(w_low, s_high) + dot(w_high, s_low))
                now = keep[c, i]
                S[c, XB + x, YB : YB + ny, :] = now + relax * (bound - now)
            return 0

        keep = mean
        lax.fori_loop(0, BAND, row, 0)

    @pl.when(g == 1)
    def _():
        restrict((0,))
        fb_copy(0).start()
        x_low, x_high = a == 0, a == cx - 1
        y_low, y_high = b == 0, b == cy - 1

        @pl.when(x_low)
        def _():
            for c in range(3):
                mean[c, 0:BAND] = S[c, XB : XB + BAND, YB : YB + ny, :]

        @pl.when(x_high)
        def _():
            for c in range(3):
                mean[c, 0:BAND] = S[c, XB + nx - BAND : XB + nx, YB : YB + ny, :]

        @pl.when(x_low | x_high)
        def _():
            xstrip_pad = jnp.zeros((3, 3, 8, lev), F32)

            @pl.when(y_low)
            def _():
                xstrip[:, :, 0:8, :] = xstrip_pad

            if (cy - 1) % 3 == 2:

                @pl.when(y_high)
                def _():
                    xstrip[:, :, ty + 8 : ty + 16, :] = xstrip_pad

        @pl.when(y_low | y_high)
        def _():
            @pl.when(x_low)
            def _():
                ystrip[:, 0:1] = jnp.zeros((3, 1, 8, lev), F32)

            if (cx - 1) % 3 == 2:

                @pl.when(x_high)
                def _():
                    ystrip[:, tx + 1 : tx + 2] = jnp.zeros((3, 1, 8, lev), F32)

            wait_strips(1, a, cx, y_windows)

        @pl.when(y_low)
        def _():
            y_edge(0, 0)

        @pl.when(y_high)
        def _():
            y_edge(ny - 8, ty - 8)

        @pl.when(x_low | x_high)
        def _():
            wait_strips(0, b, cy, x_windows)

        @pl.when(x_low)
        def _():
            x_edge(0, 0)

        @pl.when(x_high)
        def _():
            x_edge(nx - BAND, tx - 3)

        for c in range(3):
            fb_copy(c).wait_send()

    @pl.when(g == 0)
    def _():
        for on, copy in strip_copies():
            @pl.when(on)
            def _():
                copy.start()
        for on, copy in strip_copies():
            @pl.when(on)
            def _():
                copy.wait_send()
        for i in range(3):
            for j in range(3):
                there = (
                    (a >= fx) & (b >= fy) & (3 * (a - fx) + i < cx) & (3 * (b - fy) + j < cy)
                )

                @pl.when(there)
                def _():
                    for c in (1, 2, 0):
                        piece = fb.at[3 * i + j, c]
                        pltpu.make_async_remote_copy(
                            src_ref=piece, dst_ref=piece, send_sem=fb_send.at[c],
                            recv_sem=fb_recv.at[3 * i + j, c], device_id=(g, a, b),
                            device_id_type=MESH,
                        ).wait_recv()
                        at = (c, slice(XB + i * tx, XB + (i + 1) * tx),
                              slice(YB + j * ty, YB + (j + 1) * ty), slice(None))
                        now = S[at]
                        S[at] = now + FEEDBACK * (piece[...] - now)

    store = pltpu.make_async_copy(S.at[:, pl.ds(XB, nx), pl.ds(YB, ny), :], out.at[0], out_sem)
    store.start()
    for k in range(SUBS):
        for d in range(4):
            @pl.when(dirs[d][0])
            def _():
                halo_copy(k, d).wait_send()
    store.wait()


def per_device(
    state, courant, vert_inverse, interp_index, interp_weight, restrict_index, restrict_weight
):
    cx, cy = lax.axis_size("gx"), lax.axis_size("gy")
    _, _, nx, ny, lev = state.shape
    tx, ty = nx // 3, ny // 3
    vmem = lambda *shape: pltpu.VMEM(shape, F32)
    dma = pltpu.SemaphoreType.DMA
    anywhere = pl.BlockSpec(memory_space=pl.ANY)
    inside = pl.BlockSpec(memory_space=pltpu.VMEM)
    return pl.pallas_call(
        functools.partial(kernel, cx, cy),
        out_shape=jax.ShapeDtypeStruct(state.shape, F32),
        in_specs=[anywhere, anywhere] + [inside] * 5,
        out_specs=anywhere,
        scratch_shapes=[
            vmem(3, nx + 4, ny + 16, lev),
            vmem(nx + 2, ny + 16, lev),
            vmem(3, nx, ny, lev),
            vmem(2, 4, ny, lev),
            vmem(2, nx, 4, lev),
            vmem(2, 4, ny, lev),
            vmem(2, nx, 4, lev),
            vmem(SUBS - 1, 2, 2, ny, lev),
            vmem(SUBS - 1, 2, nx, 2, lev),
            vmem(SUBS - 1, 2, 2, ny, lev),
            vmem(SUBS - 1, 2, nx, 2, lev),
            vmem(3, tx, ty, lev),
            vmem(9, 3, tx, ty, lev),
            vmem(3, 3, ty + 16, lev),
            vmem(3, tx + 2, 8, lev),
            dma((2,)),
            dma((SUBS, 4)),
            dma((SUBS, 4)),
            dma((2, 2, 5)),
            dma((2, 3)),
            dma((3,)),
            dma((9, 3)),
            dma,
        ],
        compiler_params=pltpu.CompilerParams(has_side_effects=True),
        name="nest_step",
    )(state, courant, vert_inverse, interp_index, interp_weight, restrict_index, restrict_weight)


def solution(mesh):
    return jax.shard_map(
        per_device,
        mesh=mesh,
        in_specs=(
            P("grp", None, "gx", "gy", None),
            P("grp", "gx", "gy", None),
            P("grp", None, None),
            P("gx", "gy", None),
            P("gx", "gy", None),
            P("gx", "gy", None),
            P("gx", "gy", None),
        ),
        out_specs=P("grp", None, "gx", "gy", None),
        check_vma=False,
    )
```

```python
import functools

import jax
import jax.numpy as jnp
from jax import lax
from jax.experimental import pallas as pl
from jax.experimental.pallas import tpu as pltpu
from jax.sharding import PartitionSpec as P

SUBS = 4
BAND = 5
FEEDBACK = 0.5
MESH = pl.DeviceIdType.MESH
F32 = jnp.float32
XB, YB = 2, 8


def split(a):
    high = a.astype(jnp.bfloat16)
    return high, (a - high.astype(F32)).astype(jnp.bfloat16)


def dot(a, b):
    return jnp.dot(a, b, preferred_element_type=F32)


def dot3(a, b_high, b_low):
    a_high, a_low = split(a)
    return dot(a_high, b_high) + (dot(a_low, b_high) + dot(a_high, b_low))


def third(t):
    return (t * 11) >> 5


def dense(cells, shares, depth):
    places = lax.broadcasted_iota(jnp.int32, (depth, cells[0].shape[1]), 0)
    total = jnp.zeros(places.shape, F32)
    for cell, share in zip(cells, shares):
        total = total + jnp.where(places == cell, share, 0.0)
    return total.T


def kernel(
    cx, cy,
    state, courant, inverse, iidx, iwgt, ridx, rwgt,
    S,
    C, mean, wr, wx, wy, sx0, sy0, rx0, ry0, sx, sy, rx, ry, rst, fb, xstrip, ystrip,
    load_sem, halo_send, halo_recv, strip_send, strip_recv, fb_send, fb_recv,
):
    g, a, b = lax.axis_index("grp"), lax.axis_index("gx"), lax.axis_index("gy")
    nx, ny, lev = state.shape[2], state.shape[3], state.shape[4]
    tx, ty = nx // 3, ny // 3
    fx, fy = cx // 2, cy // 2

    barrier = pltpu.get_barrier_semaphore()
    greeted = []

    def greet(on, device):
        greeted.append(on)

        @pl.when(on)
        def _():
            pl.semaphore_signal(barrier, inc=1, device_id=device, device_id_type=MESH)

    greet(a > 0, (g, a - 1, b))
    greet(a < cx - 1, (g, a + 1, b))
    greet(b > 0, (g, a, b - 1))
    greet(b < cy - 1, (g, a, b + 1))
    for i in range(-1, 4):
        for j in range(-1, 4):
            child_a, child_b = 3 * (a - fx) + i, 3 * (b - fy) + j
            greet(
                (g == 0) & (a >= fx) & (b >= fy) & (child_a >= 0) & (child_a < cx)
                & (child_b >= 0) & (child_b < cy),
                (1, child_a, child_b),
            )

    def parents(place, first, count):
        own = first + place // 3
        return (
            (place >= 0, own),
            ((place % 3 == 0) & (place > 0), own - 1),
            ((place % 3 == 2) & (own + 1 < count), own + 1),
        )

    for on_a, parent_a in parents(a, fx, cx):
        for on_b, parent_b in parents(b, fy, cy):
            greet((g == 1) & on_a & on_b, (0, parent_a, parent_b))

    loads = [
        pltpu.make_async_copy(
            state.at[0], S.at[:, pl.ds(XB, nx), pl.ds(YB, ny), :], load_sem.at[0]
        ),
        pltpu.make_async_copy(
            courant.at[0], C.at[pl.ds(1, nx), pl.ds(YB, ny), :], load_sem.at[1]
        ),
    ]
    for copy in loads:
        copy.start()
    zrow = jnp.zeros((2, ny, lev), F32)
    S[0, 0:2, YB : YB + ny, :] = zrow
    S[0, XB + nx : XB + nx + 2, YB : YB + ny, :] = zrow
    S[1, 0:2, YB : YB + ny, :] = zrow
    S[1, XB + nx : XB + nx + 2, YB : YB + ny, :] = zrow
    C[0:1, YB : YB + ny, :] = zrow[0:1]
    C[nx + 1 : nx + 2, YB : YB + ny, :] = zrow[0:1]
    zcol = jnp.zeros((nx, 8, lev), F32)
    for c in (0, 2):
        S[c, XB : XB + nx, 0:YB, :] = zcol
        S[c, XB : XB + nx, YB + ny : YB + ny + 8, :] = zcol
    C[1 : 1 + nx, 0:YB, :] = zcol
    C[1 : 1 + nx, YB + ny : YB + ny + 8, :] = zcol
    m_high, m_low = split(inverse[:, 0, :])
    for copy in loads:
        copy.wait()
    pl.semaphore_wait(barrier, sum(on.astype(jnp.int32) for on in greeted))

    dirs = (
        (a > 0, a < cx - 1, (g, a - 1, b)),
        (a < cx - 1, a > 0, (g, a + 1, b)),
        (b > 0, b < cy - 1, (g, a, b - 1)),
        (b < cy - 1, b > 0, (g, a, b + 1)),
    )

    def halo_copy(k, d):
        if k == 0:
            src, dst = (sx0, rx0) if d < 2 else (sy0, ry0)
            src, dst = src.at[d % 2], dst.at[d % 2]
        else:
            src, dst = (sx, rx) if d < 2 else (sy, ry)
            src, dst = src.at[k - 1, d % 2], dst.at[k - 1, d % 2]
        return pltpu.make_async_remote_copy(
            src_ref=src, dst_ref=dst,
            send_sem=halo_send.at[k, d], recv_sem=halo_recv.at[k, d],
            device_id=dirs[d][2], device_id_type=MESH,
        )

    def exchange(k):
        cols = slice(YB, YB + ny)
        rows = slice(XB, XB + nx)
        last_x, last_y = XB + nx, YB + ny
        if k == 0:
            sx0[0, 0:2] = S[0, XB : XB + 2, cols, :]
            sx0[0, 2:3] = S[1, XB : XB + 1, cols, :]
            sx0[0, 3:4] = C[1:2, cols, :]
            sx0[1, 0:2] = S[0, last_x - 2 : last_x, cols, :]
            sx0[1, 2:3] = S[1, last_x - 1 : last_x, cols, :]
            sx0[1, 3:4] = C[nx : nx + 1, cols, :]
            sy0[0, :, 0:2] = S[0, rows, YB : YB + 2, :]
            sy0[0, :, 2:3] = S[2, rows, YB : YB + 1, :]
            sy0[0, :, 3:4] = C[1 : 1 + nx, YB : YB + 1, :]
            sy0[1, :, 0:2] = S[0, rows, last_y - 2 : last_y, :]
            sy0[1, :, 2:3] = S[2, rows, last_y - 1 : last_y, :]
            sy0[1, :, 3:4] = C[1 : 1 + nx, last_y - 1 : last_y, :]
        else:
            sx[k - 1, 0] = S[0, XB : XB + 2, cols, :]
            sx[k - 1, 1] = S[0, last_x - 2 : last_x, cols, :]
            sy[k - 1, 0] = S[0, rows, YB : YB + 2, :]
            sy[k - 1, 1] = S[0, rows, last_y - 2 : last_y, :]
        for d in range(4):
            @pl.when(dirs[d][0])
            def _():
                halo_copy(k, d).start()
        if k == 0:
            @pl.when(g == 1)
            def _():
                weights()
        for d in range(4):
            @pl.when(dirs[d][1])
            def _():
                halo_copy(k, d).wait_recv()
                if d < 2:
                    got = rx0.at[d] if k == 0 else rx.at[k - 1, d]
                    at = last_x if d == 0 else XB - 2
                    S[0, at : at + 2, cols, :] = got[0:2]
                    if k == 0:
                        at = last_x if d == 0 else XB - 1
                        S[1, at : at + 1, cols, :] = got[2:3]
                        C[at - 1 : at, cols, :] = got[3:4]
                else:
                    got = ry0.at[d - 2] if k == 0 else ry.at[k - 1, d - 2]
                    at = last_y if d == 2 else YB - 2
                    S[0, rows, at : at + 2, :] = got[:, 0:2]
                    if k == 0:
                        at = last_y if d == 2 else YB - 1
                        S[2, rows, at : at + 1, :] = got[:, 2:3]
                        C[1 : 1 + nx, at : at + 1, :] = got[:, 3:4]

    def add_mean(k, c, x, value):
        mean[c, x] = value if k == 0 else mean[c, x] + value

    def winds(k):
        def u_row(r, _):
            slope = 0.5 * (S[0, r + 1, YB : YB + ny, :] - S[0, r - 1, YB : YB + ny, :])
            S[1, r, YB : YB + ny, :] = S[1, r, YB : YB + ny, :] - C[r - 1, YB : YB + ny, :] * slope
            return 0

        u_row(XB - 1, 0)
        u_row(XB + nx, 0)

        def row(x, _):
            r = x + XB
            u_row(r, 0)
            add_mean(k, 1, x, S[1, r, YB : YB + ny, :])
            wide = slice(YB - 1, YB + ny + 1)
            slope = 0.5 * (S[0, r, YB : YB + ny + 2, :] - S[0, r, YB - 2 : YB + ny, :])
            S[2, r, wide, :] = S[2, r, wide, :] - C[x + 1, wide, :] * slope
            add_mean(k, 2, x, S[2, r, YB : YB + ny, :])
            return 0

        lax.fori_loop(0, nx, row, 0)

    def press(k):
        group = 12

        def rows(i, _):
            parts = []
            for j in range(group):
                x = i * group + j
                r = x + XB
                div = 0.5 * (S[1, r + 1, YB : YB + ny, :] - S[1, r - 1, YB : YB + ny, :]) + 0.5 * (
                    S[2, r, YB + 1 : YB + ny + 1, :] - S[2, r, YB - 1 : YB + ny - 1, :]
                )
                parts.append(S[0, r, YB : YB + ny, :] - C[x + 1, YB : YB + ny, :] * div)
            solved = dot3(jnp.concatenate(parts, axis=0), m_high, m_low)
            for j in range(group):
                x = i * group + j
                new = solved[j * ny : (j + 1) * ny]
                S[0, x + XB, YB : YB + ny, :] = new
                add_mean(k, 0, x, new)
            return 0

        lax.fori_loop(0, nx // group, rows, 0)

    slot = (a % 3) * 3 + b % 3

    def fb_copy(c):
        return pltpu.make_async_remote_copy(
            src_ref=rst.at[c], dst_ref=fb.at[slot, c],
            send_sem=fb_send.at[c], recv_sem=fb_recv.at[slot, c],
            device_id=(0, fx + a // 3, fy + b // 3), device_id_type=MESH,
        )

    def restrict(comps):
        def row(u, _):
            w_high, w_low = split(wr[u])
            for c in comps:
                block = mean[c, pl.ds(3 * u, 3)].reshape(3 * ny, lev)
                b_high, b_low = split(block)
                rst[c, u] = dot(w_high, b_high) + (dot(w_low, b_high) + dot(w_high, b_low))
            return 0

        lax.fori_loop(0, tx, row, 0)

    def row_sum(rows):
        total = rows[0]
        for row in rows[1:]:
            total = total + row
        return total

    def weights():
        x_low, x_high = a == 0, a == cx - 1
        y_low, y_high = b == 0, b == cy - 1

        def restrict_row(u, _):
            terms = range(ridx.shape[0])
            w = [rwgt[k, pl.ds(u, 1), :] for k in terms]
            scale = (1.0 / SUBS) / row_sum(w)
            over = [third(ridx[k, pl.ds(u, 1), :]) for k in terms]
            v3 = 3 * lax.broadcasted_iota(jnp.int32, (1, ty), 1)
            cells = [
                over[k] * (ny - 3) + ridx[k, pl.ds(u, 1), :] + v3 for k in terms
            ]
            wr[u] = dense(cells, [part * scale for part in w], 3 * ny)
            return 0

        lax.fori_loop(0, tx, restrict_row, 0)

        def boundary_row(x, cols, origin_x, origin_y, width, depth):
            w = [iwgt[x, k : k + 1, cols] for k in range(4)]
            scale = 1.0 / row_sum(w)
            y = cols.start + lax.broadcasted_iota(jnp.int32, w[0].shape, 1)
            y3 = (y * 171) >> 9
            cells = []
            for k in range(4):
                t = iidx[x, k : k + 1, cols]
                over = third(t)
                source_x = jnp.clip(a * tx + x // 3 + over - 1, 0, cx * tx - 1) - origin_x
                source_y = jnp.clip(b * ty + y3 + (t - 3 * over) - 1, 0, cy * ty - 1) - origin_y
                cells.append(source_x * width + source_y)
            return dense(cells, [part * scale for part in w], depth)

        def y_weights(col, strip0):
            def row(x, _):
                wy[x] = boundary_row(
                    x, slice(col, col + 8), a * tx + x // 3 - 1, b * ty + strip0, 8, 24
                )
                return 0

            lax.fori_loop(0, nx, row, 0)

        def x_weights(first, strip0):
            def row(i, _):
                wx[i] = boundary_row(
                    first + i, slice(0, ny), a * tx + strip0, b * ty - 8, ty + 16, 3 * (ty + 16)
                )
                return 0

            lax.fori_loop(0, BAND, row, 0)

        @pl.when(y_low)
        def _():
            y_weights(0, 0)

        @pl.when(y_high)
        def _():
            y_weights(ny - 8, ty - 8)

        @pl.when(x_low)
        def _():
            x_weights(0, 0)

        @pl.when(x_high)
        def _():
            x_weights(nx - BAND, tx - 3)

    for k in range(SUBS):
        exchange(k)
        winds(k)
        if k == SUBS - 1:
            @pl.when(g == 1)
            def _():
                restrict((1, 2))
                fb_copy(1).start()
                fb_copy(2).start()
        press(k)

    x_windows = {-1: (0, 8, 24), 0: (0, ty + 8, 8), 1: (ty - 8, 2 * ty + 8, 0),
                 2: (2 * ty - 8, ny, 0), 3: (ny - 8, ny, 0)}
    y_windows = {-1: (0, 1, tx + 1), 0: (0, tx + 1, 1), 1: (tx - 1, 2 * tx + 1, 0),
                 2: (2 * tx - 1, nx, 0), 3: (nx - 1, nx, 0)}
    kinds = {-1: 1, 0: 0, 1: 0, 2: 0, 3: 2}

    def strip_copies():
        for side in range(2):
            edge = 0 if side == 0 else cx - 1
            at = XB if side == 0 else XB + tx * (edge % 3) + tx - 3
            for j in range(-1, 4):
                lo, hi, dst = x_windows[j]
                child = 3 * (b - fy) + j
                on = (a == fx + edge // 3) & (b >= fy) & (child >= 0) & (child < cy)
                yield on, pltpu.make_async_remote_copy(
                    src_ref=S.at[:, pl.ds(at, 3), pl.ds(YB + lo, hi - lo), :],
                    dst_ref=xstrip.at[:, :, pl.ds(dst, hi - lo), :],
                    send_sem=strip_send.at[0, side, j + 1], recv_sem=strip_recv.at[0, kinds[j]],
                    device_id=(1, edge, child), device_id_type=MESH,
                )
            edge = 0 if side == 0 else cy - 1
            at = YB if side == 0 else YB + ty * (edge % 3) + ty - 8
            for i in range(-1, 4):
                lo, hi, dst = y_windows[i]
                child = 3 * (a - fx) + i
                on = (b == fy + edge // 3) & (a >= fx) & (child >= 0) & (child < cx)
                yield on, pltpu.make_async_remote_copy(
                    src_ref=S.at[:, pl.ds(XB + lo, hi - lo), pl.ds(at, 8), :],
                    dst_ref=ystrip.at[:, pl.ds(dst, hi - lo), :, :],
                    send_sem=strip_send.at[1, side, i + 1], recv_sem=strip_recv.at[1, kinds[i]],
                    device_id=(1, child, edge), device_id_type=MESH,
                )

    def strip_wait(axis, kind, lo, hi, dst):
        if axis == 0:
            ref = xstrip.at[:, :, pl.ds(dst, hi - lo), :]
        else:
            ref = ystrip.at[:, pl.ds(dst, hi - lo), :, :]
        pltpu.make_async_remote_copy(
            src_ref=ref, dst_ref=ref, send_sem=strip_send.at[0, 0, 0],
            recv_sem=strip_recv.at[axis, kind], device_id=(g, a, b), device_id_type=MESH,
        ).wait_recv()

    def wait_strips(axis, place, count, windows):
        for i in range(3):
            @pl.when(place % 3 == i)
            def _():
                strip_wait(axis, 0, *windows[i])

        @pl.when((place % 3 == 2) & (place < count - 1))
        def _():
            strip_wait(axis, 1, *windows[-1])

        @pl.when((place % 3 == 0) & (place > 0))
        def _():
            strip_wait(axis, 2, *windows[3])

    def relax_at(x, y):
        gx, gy = a * nx + x, b * ny + y
        depth = jnp.minimum(
            jnp.minimum(gx, nx * cx - 1 - gx), jnp.minimum(gy, ny * cy - 1 - gy)
        ).astype(F32)
        return jnp.maximum(1.0 - depth / BAND, 0.0)

    def y_edge(col):
        def row(u, _):
            n = lax.broadcasted_iota(jnp.int32, (24, lev), 0)
            relax = relax_at(3 * u + (n >> 3), col + (n & 7))
            w_high, w_low = split(wy[pl.ds(3 * u, 3)].reshape(24, 24))
            for c in range(3):
                s_high, s_low = split(ystrip[c, pl.ds(u, 3)].reshape(24, lev))
                bound = dot(w_high, s_high) + (dot(w_low, s_high) + dot(w_high, s_low))
                at = (c, pl.ds(XB + 3 * u, 3), pl.ds(YB + col, 8), slice(None))
                now = S[at].reshape(24, lev)
                S[at] = (now + relax * (bound - now)).reshape(3, 8, lev)
            return 0

        lax.fori_loop(0, tx, row, 0)

    def x_edge(first):
        def row(i, _):
            x = first + i
            w_high, w_low = split(wx[i])
            relax = relax_at(x, lax.broadcasted_iota(jnp.int32, (ny, lev), 0))
            for c in range(3):
                s_high, s_low = split(xstrip[c].reshape(3 * (ty + 16), lev))
                bound = dot(w_high, s_high) + (dot(w_low, s_high) + dot(w_high, s_low))
                now = mean[c, i]
                S[c, XB + x, YB : YB + ny, :] = now + relax * (bound - now)
            return 0

        lax.fori_loop(0, BAND, row, 0)

    @pl.when(g == 1)
    def _():
        restrict((0,))
        fb_copy(0).start()
        x_low, x_high = a == 0, a == cx - 1
        y_low, y_high = b == 0, b == cy - 1

        @pl.when(x_low)
        def _():
            for c in range(3):
                mean[c, 0:BAND] = S[c, XB : XB + BAND, YB : YB + ny, :]

        @pl.when(x_high)
        def _():
            for c in range(3):
                mean[c, 0:BAND] = S[c, XB + nx - BAND : XB + nx, YB : YB + ny, :]

        @pl.when(x_low | x_high)
        def _():
            xstrip_pad = jnp.zeros((3, 3, 8, lev), F32)

            @pl.when(y_low)
            def _():
                xstrip[:, :, 0:8, :] = xstrip_pad

            if (cy - 1) % 3 == 2:

                @pl.when(y_high)
                def _():
                    xstrip[:, :, ty + 8 : ty + 16, :] = xstrip_pad

        @pl.when(y_low | y_high)
        def _():
            @pl.when(x_low)
            def _():
                ystrip[:, 0:1] = jnp.zeros((3, 1, 8, lev), F32)

            if (cx - 1) % 3 == 2:

                @pl.when(x_high)
                def _():
                    ystrip[:, tx + 1 : tx + 2] = jnp.zeros((3, 1, 8, lev), F32)

            wait_strips(1, a, cx, y_windows)

        @pl.when(y_low)
        def _():
            y_edge(0)

        @pl.when(y_high)
        def _():
            y_edge(ny - 8)

        @pl.when(x_low | x_high)
        def _():
            wait_strips(0, b, cy, x_windows)

        @pl.when(x_low)
        def _():
            x_edge(0)

        @pl.when(x_high)
        def _():
            x_edge(nx - BAND)

        for c in range(3):
            fb_copy(c).wait_send()

    @pl.when(g == 0)
    def _():
        for on, copy in strip_copies():
            @pl.when(on)
            def _():
                copy.start()
        for on, copy in strip_copies():
            @pl.when(on)
            def _():
                copy.wait_send()
        for i in range(3):
            for j in range(3):
                there = (
                    (a >= fx) & (b >= fy) & (3 * (a - fx) + i < cx) & (3 * (b - fy) + j < cy)
                )

                @pl.when(there)
                def _():
                    for c in (1, 2, 0):
                        piece = fb.at[3 * i + j, c]
                        pltpu.make_async_remote_copy(
                            src_ref=piece, dst_ref=piece, send_sem=fb_send.at[c],
                            recv_sem=fb_recv.at[3 * i + j, c], device_id=(g, a, b),
                            device_id_type=MESH,
                        ).wait_recv()
                        at = (c, slice(XB + i * tx, XB + (i + 1) * tx),
                              slice(YB + j * ty, YB + (j + 1) * ty), slice(None))
                        now = S[at]
                        S[at] = now + FEEDBACK * (piece[...] - now)

    for k in range(SUBS):
        for d in range(4):
            @pl.when(dirs[d][0])
            def _():
                halo_copy(k, d).wait_send()


def per_device(
    state, courant, vert_inverse, interp_index, interp_weight, restrict_index, restrict_weight
):
    cx, cy = lax.axis_size("gx"), lax.axis_size("gy")
    _, _, nx, ny, lev = state.shape
    tx, ty = nx // 3, ny // 3
    vmem = lambda *shape: pltpu.VMEM(shape, F32)
    dma = pltpu.SemaphoreType.DMA
    anywhere = pl.BlockSpec(memory_space=pltpu.HBM)
    inside = pl.BlockSpec(memory_space=pltpu.VMEM)
    padded = pl.pallas_call(
        functools.partial(kernel, cx, cy),
        out_shape=vmem(3, nx + 4, ny + 16, lev),
        in_specs=[anywhere, anywhere] + [inside] * 5,
        out_specs=inside,
        scratch_shapes=[
            vmem(nx + 2, ny + 16, lev),
            vmem(3, nx, ny, lev),
            vmem(tx, ty, 3 * ny),
            vmem(BAND, ny, 3 * (ty + 16)),
            vmem(nx, 8, 24),
            vmem(2, 4, ny, lev),
            vmem(2, nx, 4, lev),
            vmem(2, 4, ny, lev),
            vmem(2, nx, 4, lev),
            vmem(SUBS - 1, 2, 2, ny, lev),
            vmem(SUBS - 1, 2, nx, 2, lev),
            vmem(SUBS - 1, 2, 2, ny, lev),
            vmem(SUBS - 1, 2, nx, 2, lev),
            vmem(3, tx, ty, lev),
            vmem(9, 3, tx, ty, lev),
            vmem(3, 3, ty + 16, lev),
            vmem(3, tx + 2, 8, lev),
            dma((2,)),
            dma((SUBS, 4)),
            dma((SUBS, 4)),
            dma((2, 2, 5)),
            dma((2, 3)),
            dma((3,)),
            dma((9, 3)),
        ],
        compiler_params=pltpu.CompilerParams(
            has_side_effects=True, collective_id=0, vmem_limit_bytes=44 * 2**20
        ),
        name="nest_step",
    )(
        state, courant, vert_inverse.transpose(1, 0, 2),
        interp_index.transpose(0, 2, 1), interp_weight.transpose(0, 2, 1),
        restrict_index.transpose(2, 0, 1), restrict_weight.transpose(2, 0, 1),
    )
    return padded[None, :, XB : XB + nx, YB : YB + ny, :]


def solution(mesh):
    return jax.shard_map(
        per_device,
        mesh=mesh,
        in_specs=(
            P("grp", None, "gx", "gy", None),
            P("grp", "gx", "gy", None),
            P("grp", None, None),
            P("gx", "gy", None),
            P("gx", "gy", None),
            P("gx", "gy", None),
            P("gx", "gy", None),
        ),
        out_specs=P("grp", None, "gx", "gy", None),
        check_vma=False,
    )
```

```python
import functools

import jax
import jax.numpy as jnp
from jax import lax
from jax.experimental import pallas as pl
from jax.experimental.pallas import tpu as pltpu
from jax.sharding import PartitionSpec as P

SUBS = 4
BAND = 5
FEEDBACK = 0.5
MESH = pl.DeviceIdType.MESH
F32 = jnp.float32
XB, YB = 2, 8


def split(a):
    high = a.astype(jnp.bfloat16)
    return high, (a - high.astype(F32)).astype(jnp.bfloat16)


def dot(a, b):
    return jnp.dot(a, b, preferred_element_type=F32)


def dot3(a, b_high, b_low):
    a_high, a_low = split(a)
    return dot(a_high, b_high) + (dot(a_low, b_high) + dot(a_high, b_low))


def third(t):
    return (t * 11) >> 5


def dense(cells, shares, depth):
    places = lax.broadcasted_iota(jnp.int32, (depth, cells[0].shape[1]), 0)
    total = jnp.zeros(places.shape, F32)
    for cell, share in zip(cells, shares):
        total = total + jnp.where(places == cell, share, 0.0)
    return total.T


def kernel(
    cx, cy,
    state, courant, *rest,
):
    small, (
    S,
    C, inverse, iidx, iwgt, ridx, rwgt, mean, wr, wx, wy, sx0, sy0, rx0, ry0, sx, sy, rx, ry, rst, fb, xstrip, ystrip,
    load_sem, halo_send, halo_recv, strip_send, strip_recv, fb_send, fb_recv,
    q0, q1, q2, q3, q_send, q_recv,
    ) = rest[:5], rest[5:]
    g, a, b = lax.axis_index("grp"), lax.axis_index("gx"), lax.axis_index("gy")
    nx, ny, lev = state.shape[2], state.shape[3], state.shape[4]
    tx, ty = nx // 3, ny // 3
    fx, fy = cx // 2, cy // 2

    barrier = pltpu.get_barrier_semaphore()
    greeted = []

    def greet(on, device):
        greeted.append(on)

        @pl.when(on)
        def _():
            pl.semaphore_signal(barrier, inc=1, device_id=device, device_id_type=MESH)

    greet(a > 0, (g, a - 1, b))
    greet(a < cx - 1, (g, a + 1, b))
    greet(b > 0, (g, a, b - 1))
    greet(b < cy - 1, (g, a, b + 1))
    for i in range(-1, 4):
        for j in range(-1, 4):
            child_a, child_b = 3 * (a - fx) + i, 3 * (b - fy) + j
            greet(
                (g == 0) & (a >= fx) & (b >= fy) & (child_a >= 0) & (child_a < cx)
                & (child_b >= 0) & (child_b < cy),
                (1, child_a, child_b),
            )

    def parents(place, first, count):
        own = first + place // 3
        return (
            (place >= 0, own),
            ((place % 3 == 0) & (place > 0), own - 1),
            ((place % 3 == 2) & (own + 1 < count), own + 1),
        )

    for on_a, parent_a in parents(a, fx, cx):
        for on_b, parent_b in parents(b, fy, cy):
            greet((g == 1) & on_a & on_b, (0, parent_a, parent_b))

    def route(at_a, at_b):
        to_a, to_b = fx + at_a // 3, fy + at_b // 3
        far = (at_a != to_a) & (at_b != to_b)
        direct = (at_a == to_a) & (at_b == to_b)
        by_nest = (at_a % 3 == 1) & (at_b == to_b) & (at_a != to_a)
        over = jnp.logical_not(direct | by_nest)
        along_a = over & (at_a % 3 == 1) & far
        along_b = over & (at_a % 3 == 0) & far
        last = over & jnp.logical_not(along_a | along_b)
        return to_a, to_b, direct, by_nest, over, along_a, along_b, last

    to_a, to_b, direct, by_nest, over, along_a, along_b, last = route(a, b)
    parent, nest = g == 0, g == 1
    mid_a = 3 * (a - fx) + 1
    comes = (a >= fx) & (mid_a < cx)
    middle = route(mid_a, b)
    relay1, relay3 = parent & comes & middle[5], nest & comes & middle[3]
    relay2 = []
    for j in range(3):
        side_b = 3 * (b - fy) + j
        relay2.append((parent & (b >= fy) & (side_b < cy) & route(a, side_b)[6], side_b))
    greet(nest & over, (0, a, b))
    greet(parent & over, (1, a, b))
    greet(parent & along_a, (0, to_a, b))
    greet(relay1, (0, mid_a, b))
    greet(parent & along_b, (0, a, to_b))
    for on, side_b in relay2:
        greet(on, (0, a, side_b))
        greet(on, (0, to_a, b))
    greet(nest & by_nest, (1, to_a, b))
    greet(relay3, (1, mid_a, b))
    greet(parent & last, (0, to_a, to_b))
    greet(relay1, (0, a, to_b))
    greet(relay3, (0, a, b))
    greet(nest & direct, (0, a, b))
    for i in range(3):
        for j in range(3):
            from_a, from_b = 3 * (a - fx) + i, 3 * (b - fy) + j
            on = parent & (a >= fx) & (b >= fy) & (from_a < cx) & (from_b < cy)
            _, _, f_direct, f_nest, _, f_a, f_b, f_last = route(from_a, from_b)
            greet(on & f_direct, (1, a, b))
            greet(on & f_nest, (1, a, from_b))
            greet(on & f_a, (0, a, from_b))
            greet(on & f_b, (0, from_a, b))
            greet(on & f_last, (0, from_a, from_b))

    loads = [
        pltpu.make_async_copy(
            state.at[0], S.at[:, pl.ds(XB, nx), pl.ds(YB, ny), :], load_sem.at[0]
        ),
        pltpu.make_async_copy(
            courant.at[0], C.at[pl.ds(1, nx), pl.ds(YB, ny), :], load_sem.at[1]
        ),
    ]
    for n, (src, dst) in enumerate(zip(small, (inverse, iidx, iwgt, ridx, rwgt))):
        loads.append(pltpu.make_async_copy(src, dst, load_sem.at[2 + n]))
    for copy in loads:
        copy.start()
    zrow = jnp.zeros((2, ny, lev), F32)
    S[0, 0:2, YB : YB + ny, :] = zrow
    S[0, XB + nx : XB + nx + 2, YB : YB + ny, :] = zrow
    S[1, 0:2, YB : YB + ny, :] = zrow
    S[1, XB + nx : XB + nx + 2, YB : YB + ny, :] = zrow
    C[0:1, YB : YB + ny, :] = zrow[0:1]
    C[nx + 1 : nx + 2, YB : YB + ny, :] = zrow[0:1]
    zcol = jnp.zeros((nx, 8, lev), F32)
    for c in (0, 2):
        S[c, XB : XB + nx, 0:YB, :] = zcol
        S[c, XB : XB + nx, YB + ny : YB + ny + 8, :] = zcol
    C[1 : 1 + nx, 0:YB, :] = zcol
    C[1 : 1 + nx, YB + ny : YB + ny + 8, :] = zcol
    for copy in loads:
        copy.wait()
    m_high, m_low = split(inverse[:, 0, :])
    pl.semaphore_wait(barrier, sum(on.astype(jnp.int32) for on in greeted))

    dirs = (
        (a > 0, a < cx - 1, (g, a - 1, b)),
        (a < cx - 1, a > 0, (g, a + 1, b)),
        (b > 0, b < cy - 1, (g, a, b - 1)),
        (b < cy - 1, b > 0, (g, a, b + 1)),
    )

    def halo_copy(k, d):
        if k == 0:
            src, dst = (sx0, rx0) if d < 2 else (sy0, ry0)
            src, dst = src.at[d % 2], dst.at[d % 2]
        else:
            src, dst = (sx, rx) if d < 2 else (sy, ry)
            src, dst = src.at[k - 1, d % 2], dst.at[k - 1, d % 2]
        return pltpu.make_async_remote_copy(
            src_ref=src, dst_ref=dst,
            send_sem=halo_send.at[k, d], recv_sem=halo_recv.at[k, d],
            device_id=dirs[d][2], device_id_type=MESH,
        )

    def exchange(k):
        cols = slice(YB, YB + ny)
        rows = slice(XB, XB + nx)
        last_x, last_y = XB + nx, YB + ny
        if k == 0:
            sx0[0, 0:2] = S[0, XB : XB + 2, cols, :]
            sx0[0, 2:3] = S[1, XB : XB + 1, cols, :]
            sx0[0, 3:4] = C[1:2, cols, :]
            sx0[1, 0:2] = S[0, last_x - 2 : last_x, cols, :]
            sx0[1, 2:3] = S[1, last_x - 1 : last_x, cols, :]
            sx0[1, 3:4] = C[nx : nx + 1, cols, :]
            sy0[0, :, 0:2] = S[0, rows, YB : YB + 2, :]
            sy0[0, :, 2:3] = S[2, rows, YB : YB + 1, :]
            sy0[0, :, 3:4] = C[1 : 1 + nx, YB : YB + 1, :]
            sy0[1, :, 0:2] = S[0, rows, last_y - 2 : last_y, :]
            sy0[1, :, 2:3] = S[2, rows, last_y - 1 : last_y, :]
            sy0[1, :, 3:4] = C[1 : 1 + nx, last_y - 1 : last_y, :]
        else:
            sx[k - 1, 0] = S[0, XB : XB + 2, cols, :]
            sx[k - 1, 1] = S[0, last_x - 2 : last_x, cols, :]
            sy[k - 1, 0] = S[0, rows, YB : YB + 2, :]
            sy[k - 1, 1] = S[0, rows, last_y - 2 : last_y, :]
        for d in range(4):
            @pl.when(dirs[d][0])
            def _():
                halo_copy(k, d).start()
        if k == 0:
            @pl.when(g == 1)
            def _():
                weights()
        for d in range(4):
            @pl.when(dirs[d][1])
            def _():
                halo_copy(k, d).wait_recv()
                if d < 2:
                    got = rx0.at[d] if k == 0 else rx.at[k - 1, d]
                    at = last_x if d == 0 else XB - 2
                    S[0, at : at + 2, cols, :] = got[0:2]
                    if k == 0:
                        at = last_x if d == 0 else XB - 1
                        S[1, at : at + 1, cols, :] = got[2:3]
                        C[at - 1 : at, cols, :] = got[3:4]
                else:
                    got = ry0.at[d - 2] if k == 0 else ry.at[k - 1, d - 2]
                    at = last_y if d == 2 else YB - 2
                    S[0, rows, at : at + 2, :] = got[:, 0:2]
                    if k == 0:
                        at = last_y if d == 2 else YB - 1
                        S[2, rows, at : at + 1, :] = got[:, 2:3]
                        C[1 : 1 + nx, at : at + 1, :] = got[:, 3:4]

    def add_mean(k, c, x, value):
        mean[c, x] = value if k == 0 else mean[c, x] + value

    def winds(k):
        def u_row(r, _):
            slope = 0.5 * (S[0, r + 1, YB : YB + ny, :] - S[0, r - 1, YB : YB + ny, :])
            S[1, r, YB : YB + ny, :] = S[1, r, YB : YB + ny, :] - C[r - 1, YB : YB + ny, :] * slope
            return 0

        u_row(XB - 1, 0)
        u_row(XB + nx, 0)

        def row(x, _):
            r = x + XB
            u_row(r, 0)
            add_mean(k, 1, x, S[1, r, YB : YB + ny, :])
            wide = slice(YB - 1, YB + ny + 1)
            slope = 0.5 * (S[0, r, YB : YB + ny + 2, :] - S[0, r, YB - 2 : YB + ny, :])
            S[2, r, wide, :] = S[2, r, wide, :] - C[x + 1, wide, :] * slope
            add_mean(k, 2, x, S[2, r, YB : YB + ny, :])
            return 0

        lax.fori_loop(0, nx, row, 0)

    def press(k):
        group = 12

        def rows(i, _):
            parts = []
            for j in range(group):
                x = i * group + j
                r = x + XB
                div = 0.5 * (S[1, r + 1, YB : YB + ny, :] - S[1, r - 1, YB : YB + ny, :]) + 0.5 * (
                    S[2, r, YB + 1 : YB + ny + 1, :] - S[2, r, YB - 1 : YB + ny - 1, :]
                )
                parts.append(S[0, r, YB : YB + ny, :] - C[x + 1, YB : YB + ny, :] * div)
            solved = dot3(jnp.concatenate(parts, axis=0), m_high, m_low)
            for j in range(group):
                x = i * group + j
                new = solved[j * ny : (j + 1) * ny]
                S[0, x + XB, YB : YB + ny, :] = new
                add_mean(k, 0, x, new)
            return 0

        lax.fori_loop(0, nx // group, rows, 0)

    def hop(src, dst, device, send, recv):
        return pltpu.make_async_remote_copy(
            src_ref=src, dst_ref=dst, send_sem=send, recv_sem=recv,
            device_id=device, device_id_type=MESH,
        )

    def home(src, c, i, j, device, send):
        n = 3 * i + j
        return hop(src, fb.at[n, c], device, send, fb_recv.at[n, c])

    def fb_copies(c):
        mine, sem = rst.at[c], fb_send.at[c]
        return (
            (direct, home(mine, c, a % 3, b % 3, (0, a, b), sem)),
            (by_nest, hop(mine, q3.at[c], (1, to_a, b), sem, q_recv.at[5, c])),
            (over, hop(mine, q0.at[c], (0, a, b), sem, q_recv.at[0, c])),
        )

    def fb_start(c):
        for on, copy in fb_copies(c):
            @pl.when(on)
            def _():
                copy.start()

    def relays(c):
        sem0 = q_send.at[0, c]
        yield parent & over, q0.at[c], 0, (
            (along_a, hop(q0.at[c], q1.at[c], (0, to_a, b), sem0, q_recv.at[1, c])),
            (along_b, hop(q0.at[c], q2.at[b % 3, c], (0, a, to_b), sem0,
                          q_recv.at[2 + b % 3, c])),
            (last, home(q0.at[c], c, a % 3, b % 3, (0, to_a, to_b), sem0)),
        )
        yield relay1, q1.at[c], 1, (
            (relay1, home(q1.at[c], c, 1, b % 3, (0, a, to_b), q_send.at[1, c])),
        )
        for j, (on, side_b) in enumerate(relay2):
            yield on, q2.at[j, c], 2 + j, (
                (on, home(q2.at[j, c], c, 0, j, (0, to_a, b), q_send.at[2 + j, c])),
            )
        yield relay3, q3.at[c], 5, (
            (relay3, home(q3.at[c], c, 1, b % 3, (0, a, b), q_send.at[5, c])),
        )

    def pass_on():
        for c in (1, 2, 0):
            for here, buffer, n, onward in relays(c):
                @pl.when(here)
                def _():
                    hop(buffer, buffer, (g, a, b), q_send.at[n, c], q_recv.at[n, c]).wait_recv()
                    for on, copy in onward:
                        @pl.when(on)
                        def _():
                            copy.start()

    def passed_on():
        for c in (1, 2, 0):
            for here, buffer, n, onward in relays(c):
                @pl.when(here)
                def _():
                    hop(buffer, buffer, (g, a, b), q_send.at[n, c], q_recv.at[n, c]).wait_send()

    def restrict(comps):
        def row(u, _):
            w_high, w_low = split(wr[u])
            for c in comps:
                block = mean[c, pl.ds(3 * u, 3)].reshape(3 * ny, lev)
                b_high, b_low = split(block)
                rst[c, u] = dot(w_high, b_high) + (dot(w_low, b_high) + dot(w_high, b_low))
            return 0

        lax.fori_loop(0, tx, row, 0)

    def row_sum(rows):
        total = rows[0]
        for row in rows[1:]:
            total = total + row
        return total

    def weights():
        x_low, x_high = a == 0, a == cx - 1
        y_low, y_high = b == 0, b == cy - 1

        def restrict_row(u, _):
            terms = range(ridx.shape[0])
            w = [rwgt[k, pl.ds(u, 1), :] for k in terms]
            scale = (1.0 / SUBS) / row_sum(w)
            over = [third(ridx[k, pl.ds(u, 1), :]) for k in terms]
            v3 = 3 * lax.broadcasted_iota(jnp.int32, (1, ty), 1)
            cells = [
                over[k] * (ny - 3) + ridx[k, pl.ds(u, 1), :] + v3 for k in terms
            ]
            wr[u] = dense(cells, [part * scale for part in w], 3 * ny)
            return 0

        lax.fori_loop(0, tx, restrict_row, 0)

        def boundary_row(x, cols, origin_x, origin_y, width, depth):
            w = [iwgt[x, k : k + 1, cols] for k in range(4)]
            scale = 1.0 / row_sum(w)
            y = cols.start + lax.broadcasted_iota(jnp.int32, w[0].shape, 1)
            y3 = (y * 171) >> 9
            cells = []
            for k in range(4):
                t = iidx[x, k : k + 1, cols]
                over = third(t)
                source_x = jnp.clip(a * tx + x // 3 + over - 1, 0, cx * tx - 1) - origin_x
                source_y = jnp.clip(b * ty + y3 + (t - 3 * over) - 1, 0, cy * ty - 1) - origin_y
                cells.append(source_x * width + source_y)
            return dense(cells, [part * scale for part in w], depth)

        def y_weights(col, strip0):
            def row(x, _):
                wy[x] = boundary_row(
                    x, slice(col, col + 8), a * tx + x // 3 - 1, b * ty + strip0, 8, 24
                )
                return 0

            lax.fori_loop(0, nx, row, 0)

        def x_weights(first, strip0):
            def row(i, _):
                wx[i] = boundary_row(
                    first + i, slice(0, ny), a * tx + strip0, b * ty - 8, ty + 16, 3 * (ty + 16)
                )
                return 0

            lax.fori_loop(0, BAND, row, 0)

        @pl.when(y_low)
        def _():
            y_weights(0, 0)

        @pl.when(y_high)
        def _():
            y_weights(ny - 8, ty - 8)

        @pl.when(x_low)
        def _():
            x_weights(0, 0)

        @pl.when(x_high)
        def _():
            x_weights(nx - BAND, tx - 3)

    for k in range(SUBS):
        exchange(k)
        winds(k)
        if k == SUBS - 1:
            @pl.when(g == 1)
            def _():
                restrict((1, 2))
                fb_start(1)
                fb_start(2)
        press(k)

    x_windows = {-1: (0, 8, 24), 0: (0, ty + 8, 8), 1: (ty - 8, 2 * ty + 8, 0),
                 2: (2 * ty - 8, ny, 0), 3: (ny - 8, ny, 0)}
    y_windows = {-1: (0, 1, tx + 1), 0: (0, tx + 1, 1), 1: (tx - 1, 2 * tx + 1, 0),
                 2: (2 * tx - 1, nx, 0), 3: (nx - 1, nx, 0)}
    kinds = {-1: 1, 0: 0, 1: 0, 2: 0, 3: 2}

    def strip_copies():
        for side in range(2):
            edge = 0 if side == 0 else cx - 1
            at = XB if side == 0 else XB + tx * (edge % 3) + tx - 3
            for j in range(-1, 4):
                lo, hi, dst = x_windows[j]
                child = 3 * (b - fy) + j
                on = (a == fx + edge // 3) & (b >= fy) & (child >= 0) & (child < cy)
                yield on, pltpu.make_async_remote_copy(
                    src_ref=S.at[:, pl.ds(at, 3), pl.ds(YB + lo, hi - lo), :],
                    dst_ref=xstrip.at[:, :, pl.ds(dst, hi - lo), :],
                    send_sem=strip_send.at[0, side, j + 1], recv_sem=strip_recv.at[0, kinds[j]],
                    device_id=(1, edge, child), device_id_type=MESH,
                )
            edge = 0 if side == 0 else cy - 1
            at = YB if side == 0 else YB + ty * (edge % 3) + ty - 8
            for i in range(-1, 4):
                lo, hi, dst = y_windows[i]
                child = 3 * (a - fx) + i
                on = (b == fy + edge // 3) & (a >= fx) & (child >= 0) & (child < cx)
                yield on, pltpu.make_async_remote_copy(
                    src_ref=S.at[:, pl.ds(XB + lo, hi - lo), pl.ds(at, 8), :],
                    dst_ref=ystrip.at[:, pl.ds(dst, hi - lo), :, :],
                    send_sem=strip_send.at[1, side, i + 1], recv_sem=strip_recv.at[1, kinds[i]],
                    device_id=(1, child, edge), device_id_type=MESH,
                )

    def strip_wait(axis, kind, lo, hi, dst):
        if axis == 0:
            ref = xstrip.at[:, :, pl.ds(dst, hi - lo), :]
        else:
            ref = ystrip.at[:, pl.ds(dst, hi - lo), :, :]
        pltpu.make_async_remote_copy(
            src_ref=ref, dst_ref=ref, send_sem=strip_send.at[0, 0, 0],
            recv_sem=strip_recv.at[axis, kind], device_id=(g, a, b), device_id_type=MESH,
        ).wait_recv()

    def wait_strips(axis, place, count, windows):
        for i in range(3):
            @pl.when(place % 3 == i)
            def _():
                strip_wait(axis, 0, *windows[i])

        @pl.when((place % 3 == 2) & (place < count - 1))
        def _():
            strip_wait(axis, 1, *windows[-1])

        @pl.when((place % 3 == 0) & (place > 0))
        def _():
            strip_wait(axis, 2, *windows[3])

    def relax_at(x, y):
        gx, gy = a * nx + x, b * ny + y
        depth = jnp.minimum(
            jnp.minimum(gx, nx * cx - 1 - gx), jnp.minimum(gy, ny * cy - 1 - gy)
        ).astype(F32)
        return jnp.maximum(1.0 - depth / BAND, 0.0)

    def y_edge(col):
        def row(u, _):
            n = lax.broadcasted_iota(jnp.int32, (24, lev), 0)
            relax = relax_at(3 * u + (n >> 3), col + (n & 7))
            w_high, w_low = split(wy[pl.ds(3 * u, 3)].reshape(24, 24))
            for c in range(3):
                s_high, s_low = split(ystrip[c, pl.ds(u, 3)].reshape(24, lev))
                bound = dot(w_high, s_high) + (dot(w_low, s_high) + dot(w_high, s_low))
                at = (c, pl.ds(XB + 3 * u, 3), pl.ds(YB + col, 8), slice(None))
                now = S[at].reshape(24, lev)
                S[at] = (now + relax * (bound - now)).reshape(3, 8, lev)
            return 0

        lax.fori_loop(0, tx, row, 0)

    def x_edge(first):
        def row(i, _):
            x = first + i
            w_high, w_low = split(wx[i])
            relax = relax_at(x, lax.broadcasted_iota(jnp.int32, (ny, lev), 0))
            for c in range(3):
                s_high, s_low = split(xstrip[c].reshape(3 * (ty + 16), lev))
                bound = dot(w_high, s_high) + (dot(w_low, s_high) + dot(w_high, s_low))
                now = mean[c, i]
                S[c, XB + x, YB : YB + ny, :] = now + relax * (bound - now)
            return 0

        lax.fori_loop(0, BAND, row, 0)

    @pl.when(g == 1)
    def _():
        restrict((0,))
        fb_start(0)
        pass_on()
        x_low, x_high = a == 0, a == cx - 1
        y_low, y_high = b == 0, b == cy - 1

        @pl.when(x_low)
        def _():
            for c in range(3):
                mean[c, 0:BAND] = S[c, XB : XB + BAND, YB : YB + ny, :]

        @pl.when(x_high)
        def _():
            for c in range(3):
                mean[c, 0:BAND] = S[c, XB + nx - BAND : XB + nx, YB : YB + ny, :]

        @pl.when(x_low | x_high)
        def _():
            xstrip_pad = jnp.zeros((3, 3, 8, lev), F32)

            @pl.when(y_low)
            def _():
                xstrip[:, :, 0:8, :] = xstrip_pad

            if (cy - 1) % 3 == 2:

                @pl.when(y_high)
                def _():
                    xstrip[:, :, ty + 8 : ty + 16, :] = xstrip_pad

        @pl.when(y_low | y_high)
        def _():
            @pl.when(x_low)
            def _():
                ystrip[:, 0:1] = jnp.zeros((3, 1, 8, lev), F32)

            if (cx - 1) % 3 == 2:

                @pl.when(x_high)
                def _():
                    ystrip[:, tx + 1 : tx + 2] = jnp.zeros((3, 1, 8, lev), F32)

            wait_strips(1, a, cx, y_windows)

        @pl.when(y_low)
        def _():
            y_edge(0)

        @pl.when(y_high)
        def _():
            y_edge(ny - 8)

        @pl.when(x_low | x_high)
        def _():
            wait_strips(0, b, cy, x_windows)

        @pl.when(x_low)
        def _():
            x_edge(0)

        @pl.when(x_high)
        def _():
            x_edge(nx - BAND)

        for c in range(3):
            hop(rst.at[c], rst.at[c], (g, a, b), fb_send.at[c], q_recv.at[0, c]).wait_send()

    @pl.when(g == 0)
    def _():
        for on, copy in strip_copies():
            @pl.when(on)
            def _():
                copy.start()
        pass_on()
        for on, copy in strip_copies():
            @pl.when(on)
            def _():
                copy.wait_send()
        for i in range(3):
            for j in range(3):
                there = (
                    (a >= fx) & (b >= fy) & (3 * (a - fx) + i < cx) & (3 * (b - fy) + j < cy)
                )

                @pl.when(there)
                def _():
                    for c in (1, 2, 0):
                        piece = fb.at[3 * i + j, c]
                        pltpu.make_async_remote_copy(
                            src_ref=piece, dst_ref=piece, send_sem=fb_send.at[c],
                            recv_sem=fb_recv.at[3 * i + j, c], device_id=(g, a, b),
                            device_id_type=MESH,
                        ).wait_recv()
                        at = (c, slice(XB + i * tx, XB + (i + 1) * tx),
                              slice(YB + j * ty, YB + (j + 1) * ty), slice(None))
                        now = S[at]
                        S[at] = now + FEEDBACK * (piece[...] - now)

    for k in range(SUBS):
        for d in range(4):
            @pl.when(dirs[d][0])
            def _():
                halo_copy(k, d).wait_send()
    passed_on()


def per_device(
    state, courant, vert_inverse, interp_index, interp_weight, restrict_index, restrict_weight
):
    cx, cy = lax.axis_size("gx"), lax.axis_size("gy")
    _, _, nx, ny, lev = state.shape
    tx, ty = nx // 3, ny // 3
    vmem = lambda *shape: pltpu.VMEM(shape, F32)
    dma = pltpu.SemaphoreType.DMA
    anywhere = pl.BlockSpec(memory_space=pltpu.HBM)
    inside = pl.BlockSpec(memory_space=pltpu.VMEM)
    padded = pl.pallas_call(
        functools.partial(kernel, cx, cy),
        out_shape=vmem(3, nx + 4, ny + 16, lev),
        in_specs=[anywhere] * 7,
        out_specs=inside,
        scratch_shapes=[
            vmem(nx + 2, ny + 16, lev),
            vmem(lev, 1, lev),
            pltpu.VMEM((nx, 4, ny), jnp.int32),
            vmem(nx, 4, ny),
            pltpu.VMEM((9, tx, ty), jnp.int32),
            vmem(9, tx, ty),
            vmem(3, nx, ny, lev),
            vmem(tx, ty, 3 * ny),
            vmem(BAND, ny, 3 * (ty + 16)),
            vmem(nx, 8, 24),
            vmem(2, 4, ny, lev),
            vmem(2, nx, 4, lev),
            vmem(2, 4, ny, lev),
            vmem(2, nx, 4, lev),
            vmem(SUBS - 1, 2, 2, ny, lev),
            vmem(SUBS - 1, 2, nx, 2, lev),
            vmem(SUBS - 1, 2, 2, ny, lev),
            vmem(SUBS - 1, 2, nx, 2, lev),
            vmem(3, tx, ty, lev),
            vmem(9, 3, tx, ty, lev),
            vmem(3, 3, ty + 16, lev),
            vmem(3, tx + 2, 8, lev),
            dma((7,)),
            dma((SUBS, 4)),
            dma((SUBS, 4)),
            dma((2, 2, 5)),
            dma((2, 3)),
            dma((3,)),
            dma((9, 3)),
            vmem(3, tx, ty, lev),
            vmem(3, tx, ty, lev),
            vmem(3, 3, tx, ty, lev),
            vmem(3, tx, ty, lev),
            dma((6, 3)),
            dma((6, 3)),
        ],
        compiler_params=pltpu.CompilerParams(
            has_side_effects=True, collective_id=0, vmem_limit_bytes=67043328 - 4 * (3 * (nx + 4) * (ny + 16) * 128) - 2**14
        ),
        name="nest_step",
    )(
        state, courant, vert_inverse.transpose(1, 0, 2),
        interp_index.transpose(0, 2, 1), interp_weight.transpose(0, 2, 1),
        restrict_index.transpose(2, 0, 1), restrict_weight.transpose(2, 0, 1),
    )
    return padded[None, :, XB : XB + nx, YB : YB + ny, :]


def solution(mesh):
    return jax.shard_map(
        per_device,
        mesh=mesh,
        in_specs=(
            P("grp", None, "gx", "gy", None),
            P("grp", "gx", "gy", None),
            P("grp", None, None),
            P("gx", "gy", None),
            P("gx", "gy", None),
            P("gx", "gy", None),
            P("gx", "gy", None),
        ),
        out_specs=P("grp", None, "gx", "gy", None),
        check_vma=False,
    )
```

```python
import functools

import jax
import jax.numpy as jnp
from jax import lax
from jax.experimental import pallas as pl
from jax.experimental.pallas import tpu as pltpu
from jax.sharding import PartitionSpec as P

SUBS = 4
BAND = 5
FEEDBACK = 0.5
MESH = pl.DeviceIdType.MESH
F32 = jnp.float32
XB, YB = 2, 8


def split(a):
    high = a.astype(jnp.bfloat16)
    return high, (a - high.astype(F32)).astype(jnp.bfloat16)


def dot(a, b):
    return jnp.dot(a, b, preferred_element_type=F32)


def dot3(a, b_high, b_low):
    a_high, a_low = split(a)
    return dot(a_high, b_high) + (dot(a_low, b_high) + dot(a_high, b_low))


def third(t):
    return (t * 11) >> 5


def dense(cells, shares, depth):
    places = lax.broadcasted_iota(jnp.int32, (depth, cells[0].shape[1]), 0)
    total = jnp.zeros(places.shape, F32)
    for cell, share in zip(cells, shares):
        total = total + jnp.where(places == cell, share, 0.0)
    return total.T


def kernel(
    cx, cy,
    state, courant, *rest,
):
    small, (
    S,
    C, inverse, iidx, iwgt, ridx, rwgt, mean, wr, wx, wy, sx0, sy0, rx0, ry0, sx, sy, rx, ry, rst, fb, xstrip, ystrip,
    load_sem, halo_send, halo_recv, strip_send, strip_recv, fb_send, fb_recv,
    q0, q1, q2, q3, q_send, q_recv,
    ) = rest[:5], rest[5:]
    g, a, b = lax.axis_index("grp"), lax.axis_index("gx"), lax.axis_index("gy")
    nx, ny, lev = state.shape[2], state.shape[3], state.shape[4]
    tx, ty = nx // 3, ny // 3
    fx, fy = cx // 2, cy // 2

    barrier = pltpu.get_barrier_semaphore()
    greeted = []

    def greet(on, device):
        greeted.append(on)

        @pl.when(on)
        def _():
            pl.semaphore_signal(barrier, inc=1, device_id=device, device_id_type=MESH)

    greet(a > 0, (g, a - 1, b))
    greet(a < cx - 1, (g, a + 1, b))
    greet(b > 0, (g, a, b - 1))
    greet(b < cy - 1, (g, a, b + 1))
    for i in range(-1, 4):
        for j in range(-1, 4):
            child_a, child_b = 3 * (a - fx) + i, 3 * (b - fy) + j
            greet(
                (g == 0) & (a >= fx) & (b >= fy) & (child_a >= 0) & (child_a < cx)
                & (child_b >= 0) & (child_b < cy),
                (1, child_a, child_b),
            )

    def parents(place, first, count):
        own = first + place // 3
        return (
            (place >= 0, own),
            ((place % 3 == 0) & (place > 0), own - 1),
            ((place % 3 == 2) & (own + 1 < count), own + 1),
        )

    for on_a, parent_a in parents(a, fx, cx):
        for on_b, parent_b in parents(b, fy, cy):
            greet((g == 1) & on_a & on_b, (0, parent_a, parent_b))

    def route(at_a, at_b):
        to_a, to_b = fx + at_a // 3, fy + at_b // 3
        far = (at_a != to_a) & (at_b != to_b)
        direct = (at_a == to_a) & (at_b == to_b)
        by_nest = (at_a % 3 == 1) & (at_b == to_b) & (at_a != to_a)
        over = jnp.logical_not(direct | by_nest)
        along_a = over & (at_a % 3 == 1) & far
        along_b = over & (at_a % 3 == 0) & far
        last = over & jnp.logical_not(along_a | along_b)
        return to_a, to_b, direct, by_nest, over, along_a, along_b, last

    to_a, to_b, direct, by_nest, over, along_a, along_b, last = route(a, b)
    parent, nest = g == 0, g == 1
    mid_a = 3 * (a - fx) + 1
    comes = (a >= fx) & (mid_a < cx)
    middle = route(mid_a, b)
    relay1, relay3 = parent & comes & middle[5], nest & comes & middle[3]
    relay2 = []
    for j in range(3):
        side_b = 3 * (b - fy) + j
        relay2.append((parent & (b >= fy) & (side_b < cy) & route(a, side_b)[6], side_b))
    greet(nest & over, (0, a, b))
    greet(parent & over, (1, a, b))
    greet(parent & along_a, (0, to_a, b))
    greet(relay1, (0, mid_a, b))
    greet(parent & along_b, (0, a, to_b))
    for on, side_b in relay2:
        greet(on, (0, a, side_b))
        greet(on, (0, to_a, b))
    greet(nest & by_nest, (1, to_a, b))
    greet(relay3, (1, mid_a, b))
    greet(parent & last, (0, to_a, to_b))
    greet(relay1, (0, a, to_b))
    greet(relay3, (0, a, b))
    greet(nest & direct, (0, a, b))
    for i in range(3):
        for j in range(3):
            from_a, from_b = 3 * (a - fx) + i, 3 * (b - fy) + j
            on = parent & (a >= fx) & (b >= fy) & (from_a < cx) & (from_b < cy)
            _, _, f_direct, f_nest, _, f_a, f_b, f_last = route(from_a, from_b)
            greet(on & f_direct, (1, a, b))
            greet(on & f_nest, (1, a, from_b))
            greet(on & f_a, (0, a, from_b))
            greet(on & f_b, (0, from_a, b))
            greet(on & f_last, (0, from_a, from_b))

    loads = [
        pltpu.make_async_copy(
            state.at[0], S.at[:, pl.ds(XB, nx), pl.ds(YB, ny), :], load_sem.at[0]
        ),
        pltpu.make_async_copy(
            courant.at[0], C.at[pl.ds(1, nx), pl.ds(YB, ny), :], load_sem.at[1]
        ),
    ]
    for n, (src, dst) in enumerate(zip(small, (inverse, iidx, iwgt, ridx, rwgt))):
        loads.append(pltpu.make_async_copy(src, dst, load_sem.at[2 + n]))
    for copy in loads:
        copy.start()
    zrow = jnp.zeros((2, ny, lev), F32)
    S[0, 0:2, YB : YB + ny, :] = zrow
    S[0, XB + nx : XB + nx + 2, YB : YB + ny, :] = zrow
    S[1, 0:2, YB : YB + ny, :] = zrow
    S[1, XB + nx : XB + nx + 2, YB : YB + ny, :] = zrow
    C[0:1, YB : YB + ny, :] = zrow[0:1]
    C[nx + 1 : nx + 2, YB : YB + ny, :] = zrow[0:1]
    zcol = jnp.zeros((nx, 8, lev), F32)
    for c in (0, 2):
        S[c, XB : XB + nx, 0:YB, :] = zcol
        S[c, XB : XB + nx, YB + ny : YB + ny + 8, :] = zcol
    C[1 : 1 + nx, 0:YB, :] = zcol
    C[1 : 1 + nx, YB + ny : YB + ny + 8, :] = zcol
    for copy in loads:
        copy.wait()
    m_high, m_low = split(inverse[:, 0, :])
    pl.semaphore_wait(barrier, sum(on.astype(jnp.int32) for on in greeted))

    dirs = (
        (a > 0, a < cx - 1, (g, a - 1, b)),
        (a < cx - 1, a > 0, (g, a + 1, b)),
        (b > 0, b < cy - 1, (g, a, b - 1)),
        (b < cy - 1, b > 0, (g, a, b + 1)),
    )

    def halo_copy(k, d):
        if k == 0:
            src, dst = (sx0, rx0) if d < 2 else (sy0, ry0)
            src, dst = src.at[d % 2], dst.at[d % 2]
        else:
            src, dst = (sx, rx) if d < 2 else (sy, ry)
            src, dst = src.at[k - 1, d % 2], dst.at[k - 1, d % 2]
        return pltpu.make_async_remote_copy(
            src_ref=src, dst_ref=dst,
            send_sem=halo_send.at[k, d], recv_sem=halo_recv.at[k, d],
            device_id=dirs[d][2], device_id_type=MESH,
        )

    def exchange(k):
        cols = slice(YB, YB + ny)
        rows = slice(XB, XB + nx)
        last_x, last_y = XB + nx, YB + ny
        if k == 0:
            sx0[0, 0:2] = S[0, XB : XB + 2, cols, :]
            sx0[0, 2:3] = S[1, XB : XB + 1, cols, :]
            sx0[0, 3:4] = C[1:2, cols, :]
            sx0[1, 0:2] = S[0, last_x - 2 : last_x, cols, :]
            sx0[1, 2:3] = S[1, last_x - 1 : last_x, cols, :]
            sx0[1, 3:4] = C[nx : nx + 1, cols, :]
            sy0[0, :, 0:2] = S[0, rows, YB : YB + 2, :]
            sy0[0, :, 2:3] = S[2, rows, YB : YB + 1, :]
            sy0[0, :, 3:4] = C[1 : 1 + nx, YB : YB + 1, :]
            sy0[1, :, 0:2] = S[0, rows, last_y - 2 : last_y, :]
            sy0[1, :, 2:3] = S[2, rows, last_y - 1 : last_y, :]
            sy0[1, :, 3:4] = C[1 : 1 + nx, last_y - 1 : last_y, :]
        else:
            sx[k - 1, 0] = S[0, XB : XB + 2, cols, :]
            sx[k - 1, 1] = S[0, last_x - 2 : last_x, cols, :]
            sy[k - 1, 0] = S[0, rows, YB : YB + 2, :]
            sy[k - 1, 1] = S[0, rows, last_y - 2 : last_y, :]
        for d in range(4):
            @pl.when(dirs[d][0])
            def _():
                halo_copy(k, d).start()
        if k == 0:
            @pl.when(g == 1)
            def _():
                weights()
        for d in range(4):
            @pl.when(dirs[d][1])
            def _():
                halo_copy(k, d).wait_recv()
                if d < 2:
                    got = rx0.at[d] if k == 0 else rx.at[k - 1, d]
                    at = last_x if d == 0 else XB - 2
                    S[0, at : at + 2, cols, :] = got[0:2]
                    if k == 0:
                        at = last_x if d == 0 else XB - 1
                        S[1, at : at + 1, cols, :] = got[2:3]
                        C[at - 1 : at, cols, :] = got[3:4]
                else:
                    got = ry0.at[d - 2] if k == 0 else ry.at[k - 1, d - 2]
                    at = last_y if d == 2 else YB - 2
                    S[0, rows, at : at + 2, :] = got[:, 0:2]
                    if k == 0:
                        at = last_y if d == 2 else YB - 1
                        S[2, rows, at : at + 1, :] = got[:, 2:3]
                        C[1 : 1 + nx, at : at + 1, :] = got[:, 3:4]

    def add_mean(k, c, x, value):
        mean[c, x] = value if k == 0 else mean[c, x] + value

    def winds(k):
        def u_row(r, _):
            slope = 0.5 * (S[0, r + 1, YB : YB + ny, :] - S[0, r - 1, YB : YB + ny, :])
            S[1, r, YB : YB + ny, :] = S[1, r, YB : YB + ny, :] - C[r - 1, YB : YB + ny, :] * slope
            return 0

        u_row(XB - 1, 0)
        u_row(XB + nx, 0)

        cols, wide = slice(YB, YB + ny), slice(YB - 1, YB + ny + 1)
        group = 4

        def rows(i, _):
            new = []
            for j in range(group):
                x = i * group + j
                r = x + XB
                slope = 0.5 * (S[0, r + 1, cols, :] - S[0, r - 1, cols, :])
                u = S[1, r, cols, :] - C[x + 1, cols, :] * slope
                slope = 0.5 * (S[0, r, YB : YB + ny + 2, :] - S[0, r, YB - 2 : YB + ny, :])
                v = S[2, r, wide, :] - C[x + 1, wide, :] * slope
                new.append((x, u, v))
            for x, u, v in new:
                S[1, x + XB, cols, :] = u
                S[2, x + XB, wide, :] = v
                add_mean(k, 1, x, u)
                add_mean(k, 2, x, v[1 : ny + 1])
            return 0

        lax.fori_loop(0, nx // group, rows, 0)

    def press(k):
        group = 12

        def rows(i, _):
            parts = []
            for j in range(group):
                x = i * group + j
                r = x + XB
                div = 0.5 * (S[1, r + 1, YB : YB + ny, :] - S[1, r - 1, YB : YB + ny, :]) + 0.5 * (
                    S[2, r, YB + 1 : YB + ny + 1, :] - S[2, r, YB - 1 : YB + ny - 1, :]
                )
                parts.append(S[0, r, YB : YB + ny, :] - C[x + 1, YB : YB + ny, :] * div)
            solved = dot3(jnp.concatenate(parts, axis=0), m_high, m_low)
            for j in range(group):
                x = i * group + j
                new = solved[j * ny : (j + 1) * ny]
                S[0, x + XB, YB : YB + ny, :] = new
                add_mean(k, 0, x, new)
            return 0

        lax.fori_loop(0, nx // group, rows, 0)

    def hop(src, dst, device, send, recv):
        return pltpu.make_async_remote_copy(
            src_ref=src, dst_ref=dst, send_sem=send, recv_sem=recv,
            device_id=device, device_id_type=MESH,
        )

    def home(src, c, i, j, device, send):
        n = 3 * i + j
        return hop(src, fb.at[n, c], device, send, fb_recv.at[n, c])

    def fb_copies(c):
        mine, sem = rst.at[c], fb_send.at[c]
        return (
            (direct, home(mine, c, a % 3, b % 3, (0, a, b), sem)),
            (by_nest, hop(mine, q3.at[c], (1, to_a, b), sem, q_recv.at[5, c])),
            (over, hop(mine, q0.at[c], (0, a, b), sem, q_recv.at[0, c])),
        )

    def fb_start(c):
        for on, copy in fb_copies(c):
            @pl.when(on)
            def _():
                copy.start()

    def relays(c):
        sem0 = q_send.at[0, c]
        yield parent & over, q0.at[c], 0, (
            (along_a, hop(q0.at[c], q1.at[c], (0, to_a, b), sem0, q_recv.at[1, c])),
            (along_b, hop(q0.at[c], q2.at[b % 3, c], (0, a, to_b), sem0,
                          q_recv.at[2 + b % 3, c])),
            (last, home(q0.at[c], c, a % 3, b % 3, (0, to_a, to_b), sem0)),
        )
        yield relay1, q1.at[c], 1, (
            (relay1, home(q1.at[c], c, 1, b % 3, (0, a, to_b), q_send.at[1, c])),
        )
        for j, (on, side_b) in enumerate(relay2):
            yield on, q2.at[j, c], 2 + j, (
                (on, home(q2.at[j, c], c, 0, j, (0, to_a, b), q_send.at[2 + j, c])),
            )
        yield relay3, q3.at[c], 5, (
            (relay3, home(q3.at[c], c, 1, b % 3, (0, a, b), q_send.at[5, c])),
        )

    def pass_on():
        for c in (1, 2, 0):
            for here, buffer, n, onward in relays(c):
                @pl.when(here)
                def _():
                    hop(buffer, buffer, (g, a, b), q_send.at[n, c], q_recv.at[n, c]).wait_recv()
                    for on, copy in onward:
                        @pl.when(on)
                        def _():
                            copy.start()

    def passed_on():
        for c in (1, 2, 0):
            for here, buffer, n, onward in relays(c):
                @pl.when(here)
                def _():
                    hop(buffer, buffer, (g, a, b), q_send.at[n, c], q_recv.at[n, c]).wait_send()

    def restrict(comps):
        group = 4

        def rows(i, _):
            new = []
            for j in range(group):
                u = i * group + j
                w_high, w_low = split(wr[u])
                for c in comps:
                    block = mean[c, pl.ds(3 * u, 3)].reshape(3 * ny, lev)
                    b_high, b_low = split(block)
                    both = dot(w_high, b_high) + (dot(w_low, b_high) + dot(w_high, b_low))
                    new.append((c, u, both))
            for c, u, both in new:
                rst[c, u] = both
            return 0

        lax.fori_loop(0, tx // group, rows, 0)

    def row_sum(rows):
        total = rows[0]
        for row in rows[1:]:
            total = total + row
        return total

    def weights():
        x_low, x_high = a == 0, a == cx - 1
        y_low, y_high = b == 0, b == cy - 1

        def restrict_row(u, _):
            terms = range(ridx.shape[0])
            w = [rwgt[k, pl.ds(u, 1), :] for k in terms]
            scale = (1.0 / SUBS) / row_sum(w)
            over = [third(ridx[k, pl.ds(u, 1), :]) for k in terms]
            v3 = 3 * lax.broadcasted_iota(jnp.int32, (1, ty), 1)
            cells = [
                over[k] * (ny - 3) + ridx[k, pl.ds(u, 1), :] + v3 for k in terms
            ]
            wr[u] = dense(cells, [part * scale for part in w], 3 * ny)
            return 0

        lax.fori_loop(0, tx, restrict_row, 0)

        def boundary_row(x, cols, origin_x, origin_y, width, depth):
            w = [iwgt[x, k : k + 1, cols] for k in range(4)]
            scale = 1.0 / row_sum(w)
            y = cols.start + lax.broadcasted_iota(jnp.int32, w[0].shape, 1)
            y3 = (y * 171) >> 9
            cells = []
            for k in range(4):
                t = iidx[x, k : k + 1, cols]
                over = third(t)
                source_x = jnp.clip(a * tx + x // 3 + over - 1, 0, cx * tx - 1) - origin_x
                source_y = jnp.clip(b * ty + y3 + (t - 3 * over) - 1, 0, cy * ty - 1) - origin_y
                cells.append(source_x * width + source_y)
            return dense(cells, [part * scale for part in w], depth)

        def y_weights(col, strip0):
            def row(x, _):
                wy[x] = boundary_row(
                    x, slice(col, col + 8), a * tx + x // 3 - 1, b * ty + strip0, 8, 24
                )
                return 0

            lax.fori_loop(0, nx, row, 0)

        def x_weights(first, strip0):
            def row(i, _):
                wx[i] = boundary_row(
                    first + i, slice(0, ny), a * tx + strip0, b * ty - 8, ty + 16, 3 * (ty + 16)
                )
                return 0

            lax.fori_loop(0, BAND, row, 0)

        @pl.when(y_low)
        def _():
            y_weights(0, 0)

        @pl.when(y_high)
        def _():
            y_weights(ny - 8, ty - 8)

        @pl.when(x_low)
        def _():
            x_weights(0, 0)

        @pl.when(x_high)
        def _():
            x_weights(nx - BAND, tx - 3)

    for k in range(SUBS):
        exchange(k)
        winds(k)
        if k == SUBS - 1:
            @pl.when(g == 1)
            def _():
                restrict((1, 2))
                fb_start(1)
                fb_start(2)
        press(k)

    x_windows = {-1: (0, 8, 24), 0: (0, ty + 8, 8), 1: (ty - 8, 2 * ty + 8, 0),
                 2: (2 * ty - 8, ny, 0), 3: (ny - 8, ny, 0)}
    y_windows = {-1: (0, 1, tx + 1), 0: (0, tx + 1, 1), 1: (tx - 1, 2 * tx + 1, 0),
                 2: (2 * tx - 1, nx, 0), 3: (nx - 1, nx, 0)}
    kinds = {-1: 1, 0: 0, 1: 0, 2: 0, 3: 2}

    def strip_copies():
        for side in range(2):
            edge = 0 if side == 0 else cx - 1
            at = XB if side == 0 else XB + tx * (edge % 3) + tx - 3
            for j in range(-1, 4):
                lo, hi, dst = x_windows[j]
                child = 3 * (b - fy) + j
                on = (a == fx + edge // 3) & (b >= fy) & (child >= 0) & (child < cy)
                yield on, pltpu.make_async_remote_copy(
                    src_ref=S.at[:, pl.ds(at, 3), pl.ds(YB + lo, hi - lo), :],
                    dst_ref=xstrip.at[:, :, pl.ds(dst, hi - lo), :],
                    send_sem=strip_send.at[0, side, j + 1], recv_sem=strip_recv.at[0, kinds[j]],
                    device_id=(1, edge, child), device_id_type=MESH,
                )
            edge = 0 if side == 0 else cy - 1
            at = YB if side == 0 else YB + ty * (edge % 3) + ty - 8
            for i in range(-1, 4):
                lo, hi, dst = y_windows[i]
                child = 3 * (a - fx) + i
                on = (b == fy + edge // 3) & (a >= fx) & (child >= 0) & (child < cx)
                yield on, pltpu.make_async_remote_copy(
                    src_ref=S.at[:, pl.ds(XB + lo, hi - lo), pl.ds(at, 8), :],
                    dst_ref=ystrip.at[:, pl.ds(dst, hi - lo), :, :],
                    send_sem=strip_send.at[1, side, i + 1], recv_sem=strip_recv.at[1, kinds[i]],
                    device_id=(1, child, edge), device_id_type=MESH,
                )

    def strip_wait(axis, kind, lo, hi, dst):
        if axis == 0:
            ref = xstrip.at[:, :, pl.ds(dst, hi - lo), :]
        else:
            ref = ystrip.at[:, pl.ds(dst, hi - lo), :, :]
        pltpu.make_async_remote_copy(
            src_ref=ref, dst_ref=ref, send_sem=strip_send.at[0, 0, 0],
            recv_sem=strip_recv.at[axis, kind], device_id=(g, a, b), device_id_type=MESH,
        ).wait_recv()

    def wait_strips(axis, place, count, windows):
        for i in range(3):
            @pl.when(place % 3 == i)
            def _():
                strip_wait(axis, 0, *windows[i])

        @pl.when((place % 3 == 2) & (place < count - 1))
        def _():
            strip_wait(axis, 1, *windows[-1])

        @pl.when((place % 3 == 0) & (place > 0))
        def _():
            strip_wait(axis, 2, *windows[3])

    def relax_at(x, y):
        gx, gy = a * nx + x, b * ny + y
        depth = jnp.minimum(
            jnp.minimum(gx, nx * cx - 1 - gx), jnp.minimum(gy, ny * cy - 1 - gy)
        ).astype(F32)
        return jnp.maximum(1.0 - depth / BAND, 0.0)

    def y_edge(col):
        def row(u, _):
            n = lax.broadcasted_iota(jnp.int32, (24, lev), 0)
            relax = relax_at(3 * u + (n >> 3), col + (n & 7))
            w_high, w_low = split(wy[pl.ds(3 * u, 3)].reshape(24, 24))
            for c in range(3):
                s_high, s_low = split(ystrip[c, pl.ds(u, 3)].reshape(24, lev))
                bound = dot(w_high, s_high) + (dot(w_low, s_high) + dot(w_high, s_low))
                at = (c, pl.ds(XB + 3 * u, 3), pl.ds(YB + col, 8), slice(None))
                now = S[at].reshape(24, lev)
                S[at] = (now + relax * (bound - now)).reshape(3, 8, lev)
            return 0

        lax.fori_loop(0, tx, row, 0)

    def x_edge(first):
        def row(i, _):
            x = first + i
            w_high, w_low = split(wx[i])
            relax = relax_at(x, lax.broadcasted_iota(jnp.int32, (ny, lev), 0))
            for c in range(3):
                s_high, s_low = split(xstrip[c].reshape(3 * (ty + 16), lev))
                bound = dot(w_high, s_high) + (dot(w_low, s_high) + dot(w_high, s_low))
                now = mean[c, i]
                S[c, XB + x, YB : YB + ny, :] = now + relax * (bound - now)
            return 0

        lax.fori_loop(0, BAND, row, 0)

    @pl.when(g == 1)
    def _():
        restrict((0,))
        fb_start(0)
        pass_on()
        x_low, x_high = a == 0, a == cx - 1
        y_low, y_high = b == 0, b == cy - 1

        @pl.when(x_low)
        def _():
            for c in range(3):
                mean[c, 0:BAND] = S[c, XB : XB + BAND, YB : YB + ny, :]

        @pl.when(x_high)
        def _():
            for c in range(3):
                mean[c, 0:BAND] = S[c, XB + nx - BAND : XB + nx, YB : YB + ny, :]

        @pl.when(x_low | x_high)
        def _():
            xstrip_pad = jnp.zeros((3, 3, 8, lev), F32)

            @pl.when(y_low)
            def _():
                xstrip[:, :, 0:8, :] = xstrip_pad

            if (cy - 1) % 3 == 2:

                @pl.when(y_high)
                def _():
                    xstrip[:, :, ty + 8 : ty + 16, :] = xstrip_pad

        @pl.when(y_low | y_high)
        def _():
            @pl.when(x_low)
            def _():
                ystrip[:, 0:1] = jnp.zeros((3, 1, 8, lev), F32)

            if (cx - 1) % 3 == 2:

                @pl.when(x_high)
                def _():
                    ystrip[:, tx + 1 : tx + 2] = jnp.zeros((3, 1, 8, lev), F32)

            wait_strips(1, a, cx, y_windows)

        @pl.when(y_low)
        def _():
            y_edge(0)

        @pl.when(y_high)
        def _():
            y_edge(ny - 8)

        @pl.when(x_low | x_high)
        def _():
            wait_strips(0, b, cy, x_windows)

        @pl.when(x_low)
        def _():
            x_edge(0)

        @pl.when(x_high)
        def _():
            x_edge(nx - BAND)

        for c in range(3):
            hop(rst.at[c], rst.at[c], (g, a, b), fb_send.at[c], q_recv.at[0, c]).wait_send()

    @pl.when(g == 0)
    def _():
        for on, copy in strip_copies():
            @pl.when(on)
            def _():
                copy.start()
        pass_on()
        for on, copy in strip_copies():
            @pl.when(on)
            def _():
                copy.wait_send()
        for i in range(3):
            for j in range(3):
                there = (
                    (a >= fx) & (b >= fy) & (3 * (a - fx) + i < cx) & (3 * (b - fy) + j < cy)
                )

                @pl.when(there)
                def _():
                    for c in (1, 2, 0):
                        piece = fb.at[3 * i + j, c]
                        pltpu.make_async_remote_copy(
                            src_ref=piece, dst_ref=piece, send_sem=fb_send.at[c],
                            recv_sem=fb_recv.at[3 * i + j, c], device_id=(g, a, b),
                            device_id_type=MESH,
                        ).wait_recv()
                        at = (c, slice(XB + i * tx, XB + (i + 1) * tx),
                              slice(YB + j * ty, YB + (j + 1) * ty), slice(None))
                        now = S[at]
                        S[at] = now + FEEDBACK * (piece[...] - now)

    for k in range(SUBS):
        for d in range(4):
            @pl.when(dirs[d][0])
            def _():
                halo_copy(k, d).wait_send()
    passed_on()


def per_device(
    state, courant, vert_inverse, interp_index, interp_weight, restrict_index, restrict_weight
):
    cx, cy = lax.axis_size("gx"), lax.axis_size("gy")
    _, _, nx, ny, lev = state.shape
    tx, ty = nx // 3, ny // 3
    vmem = lambda *shape: pltpu.VMEM(shape, F32)
    dma = pltpu.SemaphoreType.DMA
    anywhere = pl.BlockSpec(memory_space=pltpu.HBM)
    inside = pl.BlockSpec(memory_space=pltpu.VMEM)
    padded = pl.pallas_call(
        functools.partial(kernel, cx, cy),
        out_shape=vmem(3, nx + 4, ny + 16, lev),
        in_specs=[anywhere] * 7,
        out_specs=inside,
        scratch_shapes=[
            vmem(nx + 2, ny + 16, lev),
            vmem(lev, 1, lev),
            pltpu.VMEM((nx, 4, ny), jnp.int32),
            vmem(nx, 4, ny),
            pltpu.VMEM((9, tx, ty), jnp.int32),
            vmem(9, tx, ty),
            vmem(3, nx, ny, lev),
            vmem(tx, ty, 3 * ny),
            vmem(BAND, ny, 3 * (ty + 16)),
            vmem(nx, 8, 24),
            vmem(2, 4, ny, lev),
            vmem(2, nx, 4, lev),
            vmem(2, 4, ny, lev),
            vmem(2, nx, 4, lev),
            vmem(SUBS - 1, 2, 2, ny, lev),
            vmem(SUBS - 1, 2, nx, 2, lev),
            vmem(SUBS - 1, 2, 2, ny, lev),
            vmem(SUBS - 1, 2, nx, 2, lev),
            vmem(3, tx, ty, lev),
            vmem(9, 3, tx, ty, lev),
            vmem(3, 3, ty + 16, lev),
            vmem(3, tx + 2, 8, lev),
            dma((7,)),
            dma((SUBS, 4)),
            dma((SUBS, 4)),
            dma((2, 2, 5)),
            dma((2, 3)),
            dma((3,)),
            dma((9, 3)),
            vmem(3, tx, ty, lev),
            vmem(3, tx, ty, lev),
            vmem(3, 3, tx, ty, lev),
            vmem(3, tx, ty, lev),
            dma((6, 3)),
            dma((6, 3)),
        ],
        compiler_params=pltpu.CompilerParams(
            has_side_effects=True, collective_id=0, vmem_limit_bytes=67043328 - 4 * (3 * (nx + 4) * (ny + 16) * 128) - 2**14
        ),
        name="nest_step",
    )(
        state, courant, vert_inverse.transpose(1, 0, 2),
        interp_index.transpose(0, 2, 1), interp_weight.transpose(0, 2, 1),
        restrict_index.transpose(2, 0, 1), restrict_weight.transpose(2, 0, 1),
    )
    return padded[None, :, XB : XB + nx, YB : YB + ny, :]


def solution(mesh):
    return jax.shard_map(
        per_device,
        mesh=mesh,
        in_specs=(
            P("grp", None, "gx", "gy", None),
            P("grp", "gx", "gy", None),
            P("grp", None, None),
            P("gx", "gy", None),
            P("gx", "gy", None),
            P("gx", "gy", None),
            P("gx", "gy", None),
        ),
        out_specs=P("grp", None, "gx", "gy", None),
        check_vma=False,
    )
```
